128 devices in a mesh: data: 1, inner: 16 (over z, y), stage: 8 (over x, core).
Axes of the slice: x: 4, y: 4, z: 4, core: 2. Of those that a mesh axis runs over, the one named last changes fastest.
Arguments:
- x: bfloat16 [8, 512, 1536], P(('data', 'stage'), 'inner')
- g: bfloat16 [8, 512, 1536], P(('data', 'stage'), 'inner')
- w1: bfloat16 [1, 8, 1536, 6144], P(None, 'stage')
- w2: bfloat16 [1, 8, 6144, 1536], P(None, 'stage')
Outputs:
- output 1: bfloat16 [8, 512, 1536], P(('data', 'stage'), 'inner')
- output 2: bfloat16 [8, 512, 1536], P(('data', 'stage'), 'inner')
- output 3: float32 [1, 8, 1536, 6144], P('data', 'stage')
- output 4: float32 [1, 8, 6144, 1536], P('data', 'stage')
All inputs are finite; a program needn't handle non-finite values.
Results may differ from the reference program's by a relative error of at most 0.02.
Values are sent between devices in bfloat16 or wider.
A program may use at most 1 GiB of HBM per device.

```python
import jax
import jax.numpy as jnp
from jax import lax

D = 1536
FF = 6144
V = 1
K = 1
STAGE = 8
MICRO = 8
B = 512

LAYERS = V * STAGE * K


def setup_inputs(seed: int = 0, part: int = 0) -> dict:
    key = jax.random.PRNGKey(seed)
    kbase, kshared = jax.random.split(key)
    kx, kg = jax.random.split(jax.random.fold_in(kbase, part))
    k1, k2 = jax.random.split(kshared)
    x = jax.random.normal(kx, (MICRO, B, D), jnp.float32).astype(jnp.bfloat16)
    g = jax.random.normal(kg, (MICRO, B, D), jnp.float32).astype(jnp.bfloat16)
    w1 = (jax.random.normal(k1, (V, STAGE * K, D, FF), jnp.float32) * D ** -0.5).astype(jnp.bfloat16)
    w2 = (jax.random.normal(k2, (V, STAGE * K, FF, D), jnp.float32) * (2.0 * (FF * LAYERS) ** -0.5)).astype(jnp.bfloat16)
    return {"x": x, "g": g, "w1": w1, "w2": w2}


def _gelu(t):
    return jax.nn.gelu(t, approximate=True)


def _layer_fwd(h, w1, w2):
    z = jnp.dot(h, w1, preferred_element_type=jnp.float32)
    a = _gelu(z).astype(jnp.bfloat16)
    u = jnp.dot(a, w2, preferred_element_type=jnp.float32)
    return (h.astype(jnp.float32) + u).astype(jnp.bfloat16)


def _layer_bwd(h, dh, w1, w2):
    z = jnp.dot(h, w1, preferred_element_type=jnp.float32)
    a32, gelu_vjp = jax.vjp(_gelu, z)
    a = a32.astype(jnp.bfloat16)
    dw2 = jnp.dot(a.T, dh, preferred_element_type=jnp.float32)
    da = jnp.dot(dh, w2.T, preferred_element_type=jnp.float32)
    dz = gelu_vjp(da)[0].astype(jnp.bfloat16)
    dw1 = jnp.dot(h.T, dz, preferred_element_type=jnp.float32)
    dh_prev = (dh.astype(jnp.float32) + jnp.dot(dz, w1.T, preferred_element_type=jnp.float32)).astype(jnp.bfloat16)
    return dh_prev, dw1, dw2


def reference(x, g, w1, w2):
    w1s = w1.reshape(LAYERS, D, FF)
    w2s = w2.reshape(LAYERS, FF, D)

    def one_micro(acc, xg):
        dw1_acc, dw2_acc = acc
        xm, gm = xg

        def fwd(h, w):
            return _layer_fwd(h, w[0], w[1]), h

        y, hs = lax.scan(fwd, xm, (w1s, w2s))

        def bwd(dh, inp):
            h, a, b = inp
            dh_prev, d1, d2 = _layer_bwd(h, dh, a, b)
            return dh_prev, (d1, d2)

        dx, (d1s, d2s) = lax.scan(bwd, gm, (hs, w1s, w2s), reverse=True)
        return (dw1_acc + d1s, dw2_acc + d2s), (y, dx)

    init = (jnp.zeros((LAYERS, D, FF), jnp.float32), jnp.zeros((LAYERS, FF, D), jnp.float32))
    (dw1, dw2), (y, dx) = lax.scan(one_micro, init, (x, g))
    return y, dx, dw1.reshape(w1.shape), dw2.reshape(w2.shape)
```

```python
import functools

import jax
import jax.numpy as jnp
from jax import lax
from jax.experimental import pallas as pl
from jax.experimental.pallas import tpu as pltpu
from jax.sharding import PartitionSpec as P

MESH = pl.DeviceIdType.MESH
BF, F32 = jnp.bfloat16, jnp.float32
NT = (((1,), (1,)), ((), ()))
C0 = 0.7978845608028654
C1 = 0.044715
VMEM_BYTES = 67043328


def gelu_parts(z):
    z2 = z * z
    t = jnp.tanh(z * (C0 + (C0 * C1) * z2))
    cdf = 0.5 + 0.5 * t
    return z * cdf, cdf + (0.5 * z) * (1.0 - t * t) * (C0 + (3.0 * C0 * C1) * z2)


def fb_kernel(x_ref, g_ref, w1_hbm, w2_hbm, y_ref, dx_ref, hall, gall,
              bufa, bufb, dg, act, hin, hout, gin, gout, tmp,
              wsem, tsem, xs, xr, gs, gr, fs, fr, bs, br, ys, yr, ds, dr, loc, ags, agr, *, ns):
    p = lax.axis_index("stage")
    q = lax.axis_index("inner")
    z, y = q // 4, q % 4
    d, f = bufa.shape
    ck = hin.shape[1]
    nmb = ns // 2
    sub = ck // nmb
    hf = ck // 2

    def at_stage(s):
        return {"data": 0, "inner": q, "stage": s}

    def at_plane(zz, yy):
        return {"data": 0, "inner": zz * 4 + yy, "stage": p}

    def rc(src, dst, ss, rs, dev):
        return pltpu.make_async_remote_copy(src_ref=src, dst_ref=dst, send_sem=ss, recv_sem=rs, device_id=dev, device_id_type=MESH)

    cw1 = pltpu.make_async_copy(w1_hbm, bufa, wsem.at[0])
    cw2 = pltpu.make_async_copy(w2_hbm, bufb, wsem.at[1])
    cw1.start()
    cw2.start()

    bar = pltpu.get_barrier_semaphore()
    for k in range(1, ns):
        pl.semaphore_signal(bar, inc=1, device_id=at_stage(lax.rem(p + k, ns)), device_id_type=MESH)
    for k in (1, 2, 3):
        pl.semaphore_signal(bar, inc=1, device_id=at_plane(lax.rem(z + k, 4), y), device_id_type=MESH)
        pl.semaphore_signal(bar, inc=1, device_id=at_plane(z, lax.rem(y + k, 4)), device_id_type=MESH)
    pl.semaphore_wait(bar, ns - 1 + 6)

    def mine(buf):
        return buf.at[p // nmb, pl.ds(pl.multiple_of(lax.rem(p, nmb) * sub, sub), sub)]

    def gather_x(s):
        return rc(x_ref, hin.at[s // nmb, pl.ds(pl.multiple_of(lax.rem(s, nmb) * sub, sub), sub)], xs, xr.at[s], at_stage(0))

    def gather_g(s):
        return rc(g_ref, gin.at[s // nmb, pl.ds(pl.multiple_of(lax.rem(s, nmb) * sub, sub), sub)], gs, gr.at[s], at_stage(ns - 1))

    @pl.when(p > 0)
    def _():
        gather_x(p).start()

    @pl.when(p < ns - 1)
    def _():
        gather_g(p).start()

    @pl.when(p == 0)
    def _():
        hin[0, :sub] = x_ref[...]

    @pl.when(p == ns - 1)
    def _():
        gin[1, ck - sub:] = g_ref[...]

    def hop_f(c):
        return rc(hout.at[c], hin.at[c], fs.at[c], fr.at[c], at_stage(lax.rem(p + 1, ns)))

    def hop_b(c):
        return rc(gout.at[c], gin.at[c], bs.at[c], br.at[c], at_stage(lax.rem(p + ns - 1, ns)))

    def put_y(c, m):
        return rc(hout.at[c, pl.ds(m * sub, sub)], y_ref, ys.at[c * nmb + m], yr, at_stage(c * nmb + m))

    def put_dx(c, m):
        return rc(gout.at[c, pl.ds(m * sub, sub)], dx_ref, ds.at[c * nmb + m], dr, at_stage(c * nmb + m))

    def blk(out, c, zz, yy):
        return out.at[zz, yy, c]

    def line(out, c, zz, yy):
        return out.at[:, yy, c] if c == 0 else out.at[zz, :, c]

    def half(ref, up, lead):
        rows = pl.ds(0, hf) if up else pl.ds(hf, hf)
        return ref.at[:, rows] if lead else ref.at[rows]

    def shift(c, first, k):
        along_z = (c == 0) == first
        return (lax.rem(z + k + 4, 4), y) if along_z else (z, lax.rem(y + k + 4, 4))

    def ag(buf, out, a, c, step, up):
        first = step in (0, 1)
        sgn = 1 if up else -1
        to = at_plane(*shift(c, first, sgn))
        j = (a * 2 + c) * 8 + step * 2 + (0 if up else 1)
        if step == 0:
            src, dst = buf.at[c], blk(out, c, z, y)
        elif step == 1:
            src = dst = half(blk(out, c, *shift(c, True, -sgn)), up, False)
        elif step == 2:
            src = dst = line(out, c, z, y)
        else:
            src = dst = half(line(out, c, *shift(c, False, -sgn)), up, True)
        return rc(src, dst, ags.at[j], agr.at[j], to)

    def own(buf, out, a, c):
        return pltpu.make_async_copy(buf.at[c], out.at[z, y, c], loc.at[a * 2 + c])

    def ag_start(buf, out, a, c, step):
        for up in (True, False):
            ag(buf, out, a, c, step, up).start()

    def ag_wait(buf, out, a, c, step):
        for up in (True, False):
            ag(buf, out, a, c, step, up).wait()

    H, G = (hin, hall, 0), (gin, gall, 1)

    def fwd(c):
        h = hin.at[c]
        rows = pl.ds(c * ck, ck)
        for j in range(0, f, 512):
            zz = jnp.dot(h[...], bufa[:, j:j + 512], preferred_element_type=F32)
            for r in range(0, ck, 32):
                a_, d_ = gelu_parts(zz[r:r + 32])
                act[r:r + 32, j:j + 512] = a_.astype(BF)
                dg[pl.ds(c * ck + r, 32), j:j + 512] = d_
        for j in range(0, d, 512):
            u = jnp.dot(act[...], bufb[:, j:j + 512], preferred_element_type=F32)
            hout[c, :, j:j + 512] = (h[:, j:j + 512].astype(F32) + u).astype(BF)

    def bwd(c):
        g = gin.at[c]
        for j in range(0, f, 512):
            da = jnp.dot(g[...], bufa[:, j:j + 512], preferred_element_type=F32)
            for r in range(0, ck, 32):
                act[r:r + 32, j:j + 512] = (da[r:r + 32] * dg[pl.ds(c * ck + r, 32), j:j + 512]).astype(BF)
        for j in range(0, d, 512):
            u = jnp.dot(act[...], bufb[:, j:j + 512], preferred_element_type=F32)
            gout[c, :, j:j + 512] = (g[:, j:j + 512].astype(F32) + u).astype(BF)

    cw1.wait()
    cw2.wait()
    for c in (0, 1):
        @pl.when(p == 0)
        def _():
            for m in range(nmb):
                if c or m:
                    gather_x(c * nmb + m).wait_recv()

        @pl.when(p > 0)
        def _():
            hop_f(c).wait_recv()

        own(*H, c).start()
        ag_start(*H, c, 0)
        if c == 1:
            own(*H, 0).wait()
            ag_wait(*H, 0, 0)
            ag_start(*H, 0, 1)
        fwd(c)

        @pl.when(p < ns - 1)
        def _():
            hop_f(c).start()

        @pl.when(p == ns - 1)
        def _():
            for m in range(nmb):
                if c * nmb + m < ns - 1:
                    put_y(c, m).start()
            if c == 1:
                pltpu.make_async_copy(hout.at[1, pl.ds(ck - sub, sub)], y_ref, yr).start()

    own(*H, 1).wait()
    ag_wait(*H, 1, 0)
    ag_start(*H, 1, 1)

    nt = 512
    def tload(i, s):
        return pltpu.make_async_copy(w1_hbm.at[:, pl.ds(pl.multiple_of(i * nt, nt), nt)], tmp.at[s], tsem.at[s])
    tload(0, 0).start()

    def t2(i, _):
        rows = pl.ds(pl.multiple_of(i * 128, 128), 128)
        bufa[:, rows] = bufb[rows, :].T
        return 0
    lax.fori_loop(0, f // 128, t2, 0)

    def t1(i, _):
        s = lax.rem(i, 2)

        @pl.when(i + 1 < f // nt)
        def _():
            tload(i + 1, 1 - s).start()
        tload(i, s).wait()
        for r in range(0, nt, 128):
            bufb[pl.ds(pl.multiple_of(i * nt + r, 128), 128), :] = tmp[s, :, r:r + 128].T
        return 0
    lax.fori_loop(0, f // nt, t1, 0)

    def ag_rest():
        for c in (0, 1):
            ag_wait(*H, c, 1)
            ag_start(*H, c, 2)
        for c in (0, 1):
            ag_wait(*H, c, 2)
            ag_start(*H, c, 3)

    @pl.when(p < ns - 2)
    def _():
        ag_rest()

    for c in (0, 1):
        @pl.when(p == ns - 1)
        def _():
            for m in range(nmb):
                if c * nmb + m < ns - 1:
                    gather_g(c * nmb + m).wait_recv()

        @pl.when(p < ns - 1)
        def _():
            hop_b(c).wait_recv()

        own(*G, c).start()
        ag_start(*G, c, 0)
        if c == 1:
            own(*G, 0).wait()
            ag_wait(*G, 0, 0)
            ag_start(*G, 0, 1)
        bwd(c)

        @pl.when(p > 0)
        def _():
            hop_b(c).start()

        @pl.when(p == 0)
        def _():
            for m in range(nmb):
                if c * nmb + m > 0:
                    put_dx(c, m).start()
            if c == 0:
                pltpu.make_async_copy(gout.at[0, pl.ds(0, sub)], dx_ref, dr).start()

    own(*G, 1).wait()
    ag_wait(*G, 1, 0)
    ag_start(*G, 1, 1)

    @pl.when(p >= ns - 2)
    def _():
        ag_rest()
    for c in (0, 1):
        ag_wait(*G, c, 1)
        ag_start(*G, c, 2)
    for c in (0, 1):
        ag_wait(*G, c, 2)
        ag_start(*G, c, 3)

    @pl.when(p > 0)
    def _():
        gather_x(p).wait_send()
        hop_b(0).wait_send()
        hop_b(1).wait_send()
        put_dx(0, 0).wait_recv()

    @pl.when(p == 0)
    def _():
        for s in range(1, ns):
            put_dx(s // nmb, s % nmb).wait_send()
        pltpu.make_async_copy(gout.at[0, pl.ds(0, sub)], dx_ref, dr).wait()

    @pl.when(p < ns - 1)
    def _():
        gather_g(p).wait_send()
        hop_f(0).wait_send()
        hop_f(1).wait_send()
        put_y(0, 0).wait_recv()

    @pl.when(p == ns - 1)
    def _():
        for s in range(ns - 1):
            put_y(s // nmb, s % nmb).wait_send()
        pltpu.make_async_copy(hout.at[1, pl.ds(ck - sub, sub)], y_ref, yr).wait()

    for c in (0, 1):
        ag_wait(*H, c, 3)
        ag_wait(*G, c, 3)


def fb(x, g, w1, w2, ns=8, ni=16):
    b, d = x.shape
    f = w1.shape[1]
    ck = b * ns // 2
    dma = pltpu.SemaphoreType.DMA
    vm = pl.BlockSpec(memory_space=pltpu.VMEM)
    hbm = pl.BlockSpec(memory_space=pl.ANY)
    allt = jax.ShapeDtypeStruct((4, 4, 2, ck, d), BF)
    y, dx, h, gg = pl.pallas_call(
        functools.partial(fb_kernel, ns=ns),
        in_specs=[vm, vm, hbm, hbm],
        out_specs=[hbm] * 4,
        out_shape=[jax.ShapeDtypeStruct((b, d), BF)] * 2 + [allt] * 2,
        scratch_shapes=[
            pltpu.VMEM((d, f), BF), pltpu.VMEM((f, d), BF), pltpu.VMEM((2 * ck, f), F32), pltpu.VMEM((ck, f), BF),
            pltpu.VMEM((2, ck, d), BF), pltpu.VMEM((2, ck, d), BF), pltpu.VMEM((2, ck, d), BF), pltpu.VMEM((2, ck, d), BF),
            pltpu.VMEM((2, d, 512), BF),
            dma((2,)), dma((2,)), dma, dma((ns,)), dma, dma((ns,)), dma((2,)), dma((2,)), dma((2,)), dma((2,)),
            dma((ns,)), dma, dma((ns,)), dma, dma((4,)), dma((32,)), dma((32,)),
        ],
        compiler_params=pltpu.CompilerParams(vmem_limit_bytes=VMEM_BYTES, collective_id=0, has_side_effects=True),
        name="fb",
    )(x, g, w1, w2)
    return y, dx, h.reshape(-1, d), gg.reshape(-1, d)


def wgrad_kernel(w1_ref, w2_ref, h_ref, g_ref, dw1_ref, dw2_ref, w1t, at, dzt, z0, z1, d0, d1, *, tc):
    t, d = h_ref.shape
    f = w2_ref.shape[0]
    n = t // tc
    zs, ds = (z0, z1), (d0, d1)
    for r in range(0, f, 128):
        w1t[r:r + 128, :] = w1_ref[:, r:r + 128].T

    def dots(i):
        rows = pl.ds(i * tc, tc)
        zs[i % 2][...] = lax.dot_general(w1t[...], h_ref[rows, :], NT, preferred_element_type=F32)
        ds[i % 2][...] = lax.dot_general(w2_ref[...], g_ref[rows, :], NT, preferred_element_type=F32)

    def elem(i):
        cols = pl.ds(i * tc, tc)
        for r in range(0, f, 32):
            a, da = gelu_parts(zs[i % 2][r:r + 32, :])
            at[r:r + 32, cols] = a.astype(BF)
            dzt[r:r + 32, cols] = (ds[i % 2][r:r + 32, :] * da).astype(BF)

    dots(0)
    for i in range(1, n):
        dots(i)
        elem(i - 1)
    elem(n - 1)

    for j in range(0, d, 512):
        cols = pl.ds(j, 512)
        p1 = jnp.dot(dzt[...], h_ref[:, cols], preferred_element_type=F32)
        for r in range(0, 512, 128):
            dw1_ref[pl.ds(j + r, 128), :] = p1[:, r:r + 128].T
        dw2_ref[:, cols] = jnp.dot(at[...], g_ref[:, cols], preferred_element_type=F32)


def wgrad(w1, w2, h, g, f=512, tc=512):
    d, ff = w1.shape
    t = h.shape[0]
    nb = ff // f
    once = pl.Buffered(1)
    return pl.pallas_call(
        functools.partial(wgrad_kernel, tc=tc),
        grid=(nb,),
        in_specs=[
            pl.BlockSpec((d, f), lambda i: (0, i)),
            pl.BlockSpec((f, d), lambda i: (i, 0)),
            pl.BlockSpec((t, d), lambda i: (0, 0), pipeline_mode=once),
            pl.BlockSpec((t, d), lambda i: (0, 0), pipeline_mode=once),
        ],
        out_specs=[pl.BlockSpec((d, f), lambda i: (0, i)), pl.BlockSpec((f, d), lambda i: (i, 0))],
        out_shape=[jax.ShapeDtypeStruct((d, ff), F32), jax.ShapeDtypeStruct((ff, d), F32)],
        scratch_shapes=[pltpu.VMEM((f, d), BF), pltpu.VMEM((f, t), BF), pltpu.VMEM((f, t), BF)] + [pltpu.VMEM((f, tc), F32)] * 4,
        compiler_params=pltpu.CompilerParams(vmem_limit_bytes=VMEM_BYTES, dimension_semantics=("arbitrary",)),
        cost_estimate=pl.CostEstimate(flops=8 * t * d * ff, bytes_accessed=12 * d * ff + 4 * t * d, transcendentals=t * ff),
        name="wgrad",
    )(w1, w2, h, g)


def solution(mesh):
    def body(x, g, w1, w2):
        w1, w2 = w1[0, 0], w2[0, 0]
        y, dx, h, gg = fb(x[0], g[0], w1, w2)
        dw1, dw2 = wgrad(w1, w2, h, gg)
        return y[None], dx[None], dw1[None, None], dw2[None, None]

    tok = P(("data", "stage"), "inner", None)
    wsp = P(None, "stage", None, None)
    dsp = P("data", "stage", None, None)
    return jax.shard_map(body, mesh=mesh, in_specs=(tok, tok, wsp, wsp), out_specs=(tok, tok, dsp, dsp), check_vma=False)
```

```python
import functools

import jax
import jax.numpy as jnp
from jax import lax
from jax.experimental import pallas as pl
from jax.experimental.pallas import tpu as pltpu
from jax.sharding import PartitionSpec as P

MESH = pl.DeviceIdType.MESH
BF, F32 = jnp.bfloat16, jnp.float32
NT = (((1,), (1,)), ((), ()))
C0 = 0.7978845608028654
C1 = 0.044715
VMEM_BYTES = 67043328
PRE = 3
NB = 9


def gelu_parts(z):
    z2 = z * z
    t = jnp.tanh(z * (C0 + (C0 * C1) * z2))
    cdf = 0.5 + 0.5 * t
    return z * cdf, cdf + (0.5 * z) * (1.0 - t * t) * (C0 + (3.0 * C0 * C1) * z2)


def fb_kernel(x_ref, g_ref, w1_hbm, w2_hbm, y_ref, dx_ref, hall, gall, zall,
              bufa, bufb, dg, act, hin, hout, gin, gout, tmp, hbuf, zb0, zb1, zb2,
              wsem, tsem, hsem, zsem, xs, xr, gs, gr, fs, fr, bs, br, ys, yr, ds, dr, loc, ags, agr, *, ns):
    p = lax.axis_index("stage")
    q = lax.axis_index("inner")
    z, y = q // 4, q % 4
    d, f = bufa.shape
    ck = hin.shape[1]
    nmb = ns // 2
    sub = ck // nmb
    hf = ck // 2

    def at_stage(s):
        return {"data": 0, "inner": q, "stage": s}

    def at_plane(zz, yy):
        return {"data": 0, "inner": zz * 4 + yy, "stage": p}

    def rc(src, dst, ss, rs, dev):
        return pltpu.make_async_remote_copy(src_ref=src, dst_ref=dst, send_sem=ss, recv_sem=rs, device_id=dev, device_id_type=MESH)

    cw1 = pltpu.make_async_copy(w1_hbm, bufa, wsem.at[0])
    cw2 = pltpu.make_async_copy(w2_hbm, bufb, wsem.at[1])
    cw1.start()
    cw2.start()

    bar = pltpu.get_barrier_semaphore()
    for k in range(1, ns):
        pl.semaphore_signal(bar, inc=1, device_id=at_stage(lax.rem(p + k, ns)), device_id_type=MESH)
    for k in (1, 2, 3):
        pl.semaphore_signal(bar, inc=1, device_id=at_plane(lax.rem(z + k, 4), y), device_id_type=MESH)
        pl.semaphore_signal(bar, inc=1, device_id=at_plane(z, lax.rem(y + k, 4)), device_id_type=MESH)
    pl.semaphore_wait(bar, ns - 1 + 6)

    def mine(buf):
        return buf.at[p // nmb, pl.ds(pl.multiple_of(lax.rem(p, nmb) * sub, sub), sub)]

    def gather_x(s):
        return rc(x_ref, hin.at[s // nmb, pl.ds(pl.multiple_of(lax.rem(s, nmb) * sub, sub), sub)], xs, xr.at[s], at_stage(0))

    def gather_g(s):
        return rc(g_ref, gin.at[s // nmb, pl.ds(pl.multiple_of(lax.rem(s, nmb) * sub, sub), sub)], gs, gr.at[s], at_stage(ns - 1))

    @pl.when(p > 0)
    def _():
        gather_x(p).start()

    @pl.when(p < ns - 1)
    def _():
        gather_g(p).start()

    @pl.when(p == 0)
    def _():
        hin[0, :sub] = x_ref[...]

    @pl.when(p == ns - 1)
    def _():
        gin[1, ck - sub:] = g_ref[...]

    def hop_f(c):
        return rc(hout.at[c], hin.at[c], fs.at[c], fr.at[c], at_stage(lax.rem(p + 1, ns)))

    def hop_b(c):
        return rc(gout.at[c], gin.at[c], bs.at[c], br.at[c], at_stage(lax.rem(p + ns - 1, ns)))

    def put_y(c, m):
        return rc(hout.at[c, pl.ds(m * sub, sub)], y_ref, ys.at[c * nmb + m], yr, at_stage(c * nmb + m))

    def put_dx(c, m):
        return rc(gout.at[c, pl.ds(m * sub, sub)], dx_ref, ds.at[c * nmb + m], dr, at_stage(c * nmb + m))

    def blk(out, c, zz, yy):
        return out.at[zz, yy, c]

    def line(out, c, zz, yy):
        return out.at[:, yy, c] if c == 0 else out.at[zz, :, c]

    def half(ref, up, lead):
        rows = pl.ds(0, hf) if up else pl.ds(hf, hf)
        return ref.at[:, rows] if lead else ref.at[rows]

    def shift(c, first, k):
        along_z = (c == 0) == first
        return (lax.rem(z + k + 4, 4), y) if along_z else (z, lax.rem(y + k + 4, 4))

    def ag(buf, out, a, c, step, up):
        first = step in (0, 1)
        sgn = 1 if up else -1
        to = at_plane(*shift(c, first, sgn))
        j = (a * 2 + c) * 8 + step * 2 + (0 if up else 1)
        if step == 0:
            src, dst = buf.at[c], blk(out, c, z, y)
        elif step == 1:
            src = dst = half(blk(out, c, *shift(c, True, -sgn)), up, False)
        elif step == 2:
            src = dst = line(out, c, z, y)
        else:
            src = dst = half(line(out, c, *shift(c, False, -sgn)), up, True)
        return rc(src, dst, ags.at[j], agr.at[j], to)

    def own(buf, out, a, c):
        return pltpu.make_async_copy(buf.at[c], out.at[z, y, c], loc.at[a * 2 + c])

    def ag_start(buf, out, a, c, step):
        for up in (True, False):
            ag(buf, out, a, c, step, up).start()

    def ag_wait(buf, out, a, c, step):
        for up in (True, False):
            ag(buf, out, a, c, step, up).wait()

    H, G = (hin, hall, 0), (gin, gall, 1)
    last = ns - 1

    def ag_go(who, step):
        for c in (0, 1):
            ag_wait(*who, c, step - 1)
            ag_start(*who, c, step)

    def ag_end(who):
        for c in (0, 1):
            ag_wait(*who, c, 3)

    def ag_in(who, c):
        for cc in (0, 1):
            @pl.when(c == cc)
            def _():
                own(*who, cc).start()
                ag_start(*who, cc, 0)

    def ag_in_end(who):
        for c in (0, 1):
            own(*who, c).wait()
        ag_go(who, 1)

    def up(c, src, k):
        for j in range(0, d, 512):
            u = jnp.dot(act[k], bufb[:, j:j + 512], preferred_element_type=F32)
            hout[c, :, j:j + 512] = (src[:, j:j + 512].astype(F32) + u).astype(BF)

    def rows_of(c, r, n):
        return pl.ds(pl.multiple_of(c * ck + r, n), n)

    def fwd(c):
        h = hin.at[c]
        for j in range(0, f, 512):
            zz = jnp.dot(h[...], bufa[:, j:j + 512], preferred_element_type=F32)
            for r in range(0, ck, 32):
                a_, d_ = gelu_parts(zz[r:r + 32])
                act[0, r:r + 32, j:j + 512] = a_.astype(BF)
                dg[rows_of(c, r, 32), j:j + 512] = d_

        @pl.when(c == 0)
        def _():
            cw2.wait()
        up(c, h, 0)

    def bwd(c):
        g = gin.at[c]
        for j in range(0, f, 512):
            da = jnp.dot(g[...], bufa[:, j:j + 512], preferred_element_type=F32)
            for r in range(0, ck, 32):
                act[0, r:r + 32, j:j + 512] = (da[r:r + 32] * dg[rows_of(c, r, 32), j:j + 512]).astype(BF)
        for j in range(0, d, 512):
            u = jnp.dot(act[0], bufb[:, j:j + 512], preferred_element_type=F32)
            gout[c, :, j:j + 512] = (g[:, j:j + 512].astype(F32) + u).astype(BF)

    def turn(c):
        h, g = hin.at[c], gin.at[c]
        for j in range(0, f, 512):
            zz = jnp.dot(h[...], bufa[:, j:j + 512], preferred_element_type=F32)
            for r in range(0, ck, 32):
                a_, d_ = gelu_parts(zz[r:r + 32])
                act[c, r:r + 32, j:j + 512] = a_.astype(BF)
                act[2, r:r + 32, j:j + 512] = (dg[rows_of(c, r, 32), j:j + 512] * d_).astype(BF)
        for j in range(0, d, 512):
            u = lax.dot_general(act[2], bufa[j:j + 512, :], NT, preferred_element_type=F32)
            gout[c, :, j:j + 512] = (g[:, j:j + 512].astype(F32) + u).astype(BF)

    cw1.wait()

    @pl.when(p < last)
    def _():
        @pl.loop(0, 2)
        def _(c):
            @pl.when(p == 0)
            def _():
                for m in range(nmb):
                    @pl.when(c * nmb + m > 0)
                    def _():
                        gather_x(c * nmb + m).wait_recv()

            @pl.when(p > 0)
            def _():
                hop_f(c).wait_recv()
            ag_in(H, c)
            fwd(c)
            hop_f(c).start()
        ag_in_end(H)

    @pl.when(p == last)
    def _():
        cw2.wait()
        for s in range(last):
            gather_g(s).wait_recv()
        for c in (0, 1):
            own(*G, c).start()
            ag_start(*G, c, 0)

        @pl.loop(0, 2)
        def _(c):
            for j in range(0, f, 512):
                dg[rows_of(c, 0, ck), j:j + 512] = lax.dot_general(gin[c], bufb[j:j + 512, :], NT, preferred_element_type=F32)
        for c in (0, 1):
            own(*G, c).wait()
        for step in (1, 2, 3):
            ag_go(G, step)

        @pl.loop(0, 2)
        def _(c):
            hop_f(c).wait_recv()
            ag_in(H, c)
            turn(c)
            hop_b(c).start()

        @pl.loop(0, 2)
        def _(c):
            up(c, hin.at[c], c)
            for m in range(nmb):
                @pl.when(c * nmb + m < last)
                def _():
                    put_y(c, m).start()
        pltpu.make_async_copy(hout.at[1, pl.ds(ck - sub, sub)], y_ref, yr).start()
        ag_in_end(H)
        ag_go(H, 2)

    @pl.when(p < last - 1)
    def _():
        ag_go(H, 2)

    nt = 512

    def tload(i, s):
        return pltpu.make_async_copy(w1_hbm.at[:, pl.ds(pl.multiple_of(i * nt, nt), nt)], tmp.at[s], tsem.at[s])
    tload(0, 0).start()

    @pl.loop(0, f // nt)
    def _(i):
        for r in range(0, nt, 128):
            rows = pl.ds(pl.multiple_of(i * nt + r, 128), 128)
            bufa[:, rows] = bufb[rows, :].T

    @pl.loop(0, f // nt)
    def _(i):
        s = lax.rem(i, 2)

        @pl.when(i + 1 < f // nt)
        def _():
            tload(i + 1, 1 - s).start()
        tload(i, s).wait()
        for r in range(0, nt, 128):
            bufb[pl.ds(pl.multiple_of(i * nt + r, 128), 128), :] = tmp[s, :, r:r + 128].T

    @pl.when(p == last - 1)
    def _():
        ag_go(H, 2)

    nf = zall.shape[0] // 512
    nt_z = zall.shape[1] // 512
    zb = (zb0, zb1, zb2)

    def hload(t):
        s = lax.rem(t, 2)
        return pltpu.make_async_copy(hall.at[t // 2, pl.ds(2 * s, 2)], hbuf.at[s], hsem.at[s])

    def zput(n, u):
        rows = pl.ds(pl.multiple_of(lax.rem(n, nf) * 512, 512), 512)
        cols = pl.ds(pl.multiple_of((n // nf) * 512, 512), 512)
        return pltpu.make_async_copy(zb[u], zall.at[rows, cols], zsem.at[u])

    def zwork(t0, t1):
        hload(t0).start()

        @pl.loop(t0, t1)
        def _(t):
            hload(t).wait()

            @pl.when(t + 1 < t1)
            def _():
                hload(t + 1).start()

            @pl.loop(0, nf // 3)
            def _(k):
                for u in range(3):
                    n = t * nf + 3 * k + u

                    @pl.when(n >= t0 * nf + 3)
                    def _():
                        zput(n - 3, u).wait()
                    rows = pl.ds(pl.multiple_of((3 * k + u) * 512, 512), 512)
                    hc = hbuf[lax.rem(t, 2)].reshape(512, d)
                    zb[u][...] = lax.dot_general(bufb[rows, :], hc, NT, preferred_element_type=F32)
                    zput(n, u).start()
        for u in range(3):
            zput(t1 * nf - 3 + u, u).wait()

    pre = jnp.where(p < 2, PRE, 0)
    mid = jnp.where(p < 2, (nt_z + PRE) // 2, nt_z // 2)

    @pl.when(p < 4)
    def _():
        ag_go(H, 3)

    @pl.when(p < 2)
    def _():
        ag_end(H)
        zwork(0, pre)

    @pl.when(p < last)
    def _():
        @pl.loop(0, 2)
        def _(c):
            hop_b(c).wait_recv()
            ag_in(G, c)
            bwd(c)

            @pl.when(p > 0)
            def _():
                hop_b(c).start()

            @pl.when(p == 0)
            def _():
                for m in range(nmb):
                    @pl.when(c * nmb + m > 0)
                    def _():
                        put_dx(c, m).start()

        @pl.when(p == 0)
        def _():
            pltpu.make_async_copy(gout.at[0, pl.ds(0, sub)], dx_ref, dr).start()
        ag_in_end(G)

    @pl.when(p >= 4)
    def _():
        ag_go(H, 3)

    @pl.when(p >= 2)
    def _():
        ag_end(H)

    @pl.when(p < last)
    def _():
        ag_go(G, 2)
    zwork(pre, mid)

    @pl.when(p < last)
    def _():
        ag_go(G, 3)
    zwork(mid, nt_z)
    ag_end(G)

    @pl.when(p > 0)
    def _():
        gather_x(p).wait_send()
        hop_b(0).wait_send()
        hop_b(1).wait_send()
        put_dx(0, 0).wait_recv()

    @pl.when(p == 0)
    def _():
        for s in range(1, ns):
            put_dx(s // nmb, s % nmb).wait_send()
        pltpu.make_async_copy(gout.at[0, pl.ds(0, sub)], dx_ref, dr).wait()

    @pl.when(p < ns - 1)
    def _():
        gather_g(p).wait_send()
        hop_f(0).wait_send()
        hop_f(1).wait_send()
        put_y(0, 0).wait_recv()

    @pl.when(p == ns - 1)
    def _():
        for s in range(ns - 1):
            put_y(s // nmb, s % nmb).wait_send()
        pltpu.make_async_copy(hout.at[1, pl.ds(ck - sub, sub)], y_ref, yr).wait()


def fb(x, g, w1, w2, nz, ns=8):
    b, d = x.shape
    f = w1.shape[1]
    ck = b * ns // 2
    dma = pltpu.SemaphoreType.DMA
    vm = pl.BlockSpec(memory_space=pltpu.VMEM)
    hbm = pl.BlockSpec(memory_space=pl.ANY)
    allt = jax.ShapeDtypeStruct((4, 4, 2, ck, d), BF)
    y, dx, h, gg, z = pl.pallas_call(
        functools.partial(fb_kernel, ns=ns),
        in_specs=[vm, vm, hbm, hbm],
        out_specs=[hbm] * 5,
        out_shape=[jax.ShapeDtypeStruct((b, d), BF)] * 2 + [allt] * 2 + [jax.ShapeDtypeStruct((nz, 32 * ck), F32)],
        scratch_shapes=[
            pltpu.VMEM((d, f), BF), pltpu.VMEM((f, d), BF), pltpu.VMEM((2 * ck, f), F32), pltpu.VMEM((3, ck, f), BF),
            pltpu.VMEM((2, ck, d), BF), pltpu.VMEM((2, ck, d), BF), pltpu.VMEM((2, ck, d), BF), pltpu.VMEM((2, ck, d), BF),
            pltpu.VMEM((2, d, 512), BF), pltpu.VMEM((2, 2, 2, ck, d), BF), pltpu.VMEM((512, 512), F32), pltpu.VMEM((512, 512), F32), pltpu.VMEM((512, 512), F32),
            dma((2,)), dma((2,)), dma((2,)), dma((3,)), dma, dma((ns,)), dma, dma((ns,)), dma((2,)), dma((2,)), dma((2,)), dma((2,)),
            dma((ns,)), dma, dma((ns,)), dma, dma((4,)), dma((32,)), dma((32,)),
        ],
        compiler_params=pltpu.CompilerParams(vmem_limit_bytes=VMEM_BYTES, collective_id=0, has_side_effects=True),
        name="fb",
    )(x, g, w1, w2)
    return y, dx, h.reshape(-1, d), gg.reshape(-1, d), z


def wgrad_kernel(z_hbm, w2_ref, h_hbm, g_hbm, dw1_ref, dw2_ref, h_ref, g_ref, at, dzt, z0, z1, d0, d1, hsem, zsem):
    b = pl.program_id(0)
    nb = pl.num_programs(0)
    t, d = h_ref.shape
    f = w2_ref.shape[0]
    tc = d0.shape[1]
    n = t // tc
    half = t // 2
    zs, ds = (z0, z1), (d0, d1)

    def zget(blk, i):
        rows = pl.ds(pl.multiple_of(blk * f, f), f)
        return pltpu.make_async_copy(z_hbm.at[rows, pl.ds(i * half, half)], zs[i], zsem.at[i])

    gget = pltpu.make_async_copy(g_hbm, g_ref, hsem.at[0])
    hget = pltpu.make_async_copy(h_hbm, h_ref, hsem.at[1])

    @pl.when(b == 0)
    def _():
        gget.start()
        zget(0, 0).start()
        zget(0, 1).start()
        hget.start()
        gget.wait()

    def dots(i):
        rows = pl.ds(i * tc, tc)
        ds[i % 2][...] = lax.dot_general(w2_ref[...], g_ref[rows, :], NT, preferred_element_type=F32)

    def elem(i):
        cols = pl.ds(i * tc, tc)
        off = (i * tc) % half
        for r in range(0, f, 32):
            a, da = gelu_parts(zs[i * tc // half][r:r + 32, off:off + tc])
            at[r:r + 32, cols] = a.astype(BF)
            dzt[r:r + 32, cols] = (ds[i % 2][r:r + 32, :] * da).astype(BF)

    zget(b, 0).wait()
    dots(0)
    for i in range(1, n // 2 + 1):
        dots(i)
        elem(i - 1)
    zget(b, 1).wait()

    @pl.when(b + 1 < nb)
    def _():
        zget(b + 1, 0).start()

    @pl.when(b == 0)
    def _():
        hget.wait()
    for i in range(n // 2 + 1, n):
        dots(i)
        elem(i - 1)
    elem(n - 1)
    for j in range(0, d, 512):
        cols = pl.ds(j, 512)
        p1 = jnp.dot(dzt[...], h_ref[:, cols], preferred_element_type=F32)
        for r in range(0, 512, 128):
            dw1_ref[pl.ds(j + r, 128), :] = p1[:, r:r + 128].T
        dw2_ref[:, cols] = jnp.dot(at[...], g_ref[:, cols], preferred_element_type=F32)

    @pl.when(b + 1 < nb)
    def _():
        zget(b + 1, 1).start()


def wgrad(z, w2, h, g, f=512, tc=512):
    ff, d = w2.shape
    t = h.shape[0]
    nb = z.shape[0] // f
    hbm = pl.BlockSpec(memory_space=pl.ANY)
    dma = pltpu.SemaphoreType.DMA
    return pl.pallas_call(
        wgrad_kernel,
        grid=(nb,),
        in_specs=[hbm, pl.BlockSpec((f, d), lambda i: (i, 0)), hbm, hbm],
        out_specs=[pl.BlockSpec((d, f), lambda i: (0, i)), pl.BlockSpec((f, d), lambda i: (i, 0))],
        out_shape=[jax.ShapeDtypeStruct((d, ff), F32), jax.ShapeDtypeStruct((ff, d), F32)],
        scratch_shapes=[pltpu.VMEM((t, d), BF)] * 2 + [pltpu.VMEM((f, t), BF)] * 2 + [pltpu.VMEM((f, t // 2), F32)] * 2 + [pltpu.VMEM((f, tc), F32)] * 2
        + [dma((2,)), dma((2,))],
        compiler_params=pltpu.CompilerParams(vmem_limit_bytes=VMEM_BYTES, dimension_semantics=("arbitrary",)),
        cost_estimate=pl.CostEstimate(flops=6 * t * d * ff, bytes_accessed=10 * d * ff + 4 * t * d + 4 * t * ff, transcendentals=t * ff),
        name="wgrad",
    )(z, w2, h, g)


def share_kernel(w1t, w2, h_hbm, g_hbm, s1, s2, h_ref, g_ref, at, dzt, hsem, gsem, *, tc):
    t = h_ref.shape[0]
    n = t // tc

    def part(src, dst, sem, i):
        rows = pl.ds(i * tc if isinstance(i, int) else pl.multiple_of(i * tc, tc), tc)
        return pltpu.make_async_copy(src.at[rows], dst.at[rows], sem.at[i])
    for i in range(n):
        part(h_hbm, h_ref, hsem, i).start()
        part(g_hbm, g_ref, gsem, i).start()

    @pl.loop(0, n)
    def _(i):
        rows = pl.ds(pl.multiple_of(i * tc, tc), tc)
        part(h_hbm, h_ref, hsem, i).wait()
        part(g_hbm, g_ref, gsem, i).wait()
        z = lax.dot_general(w1t[...], h_ref[rows, :], NT, preferred_element_type=F32)
        da = lax.dot_general(w2[...], g_ref[rows, :], NT, preferred_element_type=F32)
        a, dg = gelu_parts(z)
        at[:, rows] = a.astype(BF)
        dzt[:, rows] = (da * dg).astype(BF)

    @pl.loop(0, h_ref.shape[1] // 512)
    def _(j):
        cols = pl.ds(pl.multiple_of(j * 512, 512), 512)
        s1[:, cols] = jnp.dot(dzt[...], h_ref[:, cols], preferred_element_type=F32)
        s2[:, cols] = jnp.dot(at[...], g_ref[:, cols], preferred_element_type=F32)


def share(w1t, w2, h, g, tc=1024):
    fs, d = w2.shape
    t = h.shape[0]
    vm = pl.BlockSpec(memory_space=pltpu.VMEM)
    hbm = pl.BlockSpec(memory_space=pl.ANY)
    dma = pltpu.SemaphoreType.DMA
    return pl.pallas_call(
        functools.partial(share_kernel, tc=tc),
        in_specs=[vm, vm, hbm, hbm],
        out_specs=[vm, vm],
        out_shape=[jax.ShapeDtypeStruct((fs, d), F32)] * 2,
        scratch_shapes=[pltpu.VMEM((t, d), BF)] * 2 + [pltpu.VMEM((fs, t), BF)] * 2 + [dma((t // tc,)), dma((t // tc,))],
        compiler_params=pltpu.CompilerParams(vmem_limit_bytes=VMEM_BYTES),
        cost_estimate=pl.CostEstimate(flops=16 * t * d * fs, bytes_accessed=4 * t * d, transcendentals=t * fs),
        name="share",
    )(w1t, w2, h, g)


def finish_kernel(s1, s2, dw1_in, dw2_in, dw1, dw2):
    del dw1_in, dw2_in
    for r in range(0, s1.shape[1], 256):
        dw1[pl.ds(r, 256), :] = s1[:, r:r + 256].T
    dw2[...] = s2[...]


def finish(s1, s2, dw1, dw2, first, f=512):
    n, d = s1.shape
    hbm = pl.BlockSpec(memory_space=pl.ANY)
    row = pl.BlockSpec((f, d), lambda i: (i, 0))
    return pl.pallas_call(
        finish_kernel,
        grid=(n // f,),
        in_specs=[row, row, hbm, hbm],
        out_specs=[pl.BlockSpec((d, f), lambda i: (0, first + i)), pl.BlockSpec((f, d), lambda i: (first + i, 0))],
        out_shape=[jax.ShapeDtypeStruct(dw1.shape, F32), jax.ShapeDtypeStruct(dw2.shape, F32)],
        input_output_aliases={2: 0, 3: 1},
        compiler_params=pltpu.CompilerParams(vmem_limit_bytes=VMEM_BYTES, dimension_semantics=("arbitrary",)),
        cost_estimate=pl.CostEstimate(flops=n * d, bytes_accessed=16 * n * d, transcendentals=0),
        name="finish",
    )(s1, s2, dw1, dw2)


def solution(mesh):
    def body(x, g, w1, w2):
        w1, w2 = w1[0, 0], w2[0, 0]
        ff, d = w2.shape
        nz = NB * 512
        fs = (ff - nz) // 16
        at = nz + lax.axis_index("inner") * fs
        w1t = lax.dynamic_slice(w1, (0, at), (d, fs)).T
        w2s = lax.dynamic_slice(w2, (at, 0), (fs, d))
        y, dx, h, gg, z = fb(x[0], g[0], w1, w2, nz)
        s1, s2 = share(w1t, w2s, h, gg)
        s1 = lax.all_gather(s1, "inner", axis=0, tiled=True)
        s2 = lax.all_gather(s2, "inner", axis=0, tiled=True)
        dw1, dw2 = wgrad(z, w2, h, gg)
        dw1, dw2 = finish(s1, s2, dw1, dw2, NB)
        return y[None], dx[None], dw1[None, None], dw2[None, None]

    tok = P(("data", "stage"), "inner", None)
    wsp = P(None, "stage", None, None)
    dsp = P("data", "stage", None, None)
    return jax.shard_map(body, mesh=mesh, in_specs=(tok, tok, wsp, wsp), out_specs=(tok, tok, dsp, dsp), check_vma=False)
```

```python
import functools

import jax
import jax.numpy as jnp
from jax import lax
from jax.experimental import pallas as pl
from jax.experimental.pallas import tpu as pltpu
from jax.sharding import PartitionSpec as P

MESH = pl.DeviceIdType.MESH
BF, F32 = jnp.bfloat16, jnp.float32
NT = (((1,), (1,)), ((), ()))
C0 = 0.7978845608028654
C1 = 0.044715
VMEM_BYTES = 67043328
NB = 9


def gelu_parts(z):
    z2 = z * z
    t = jnp.tanh(z * (C0 + (C0 * C1) * z2))
    cdf = 0.5 + 0.5 * t
    return z * cdf, cdf + (0.5 * z) * (1.0 - t * t) * (C0 + (3.0 * C0 * C1) * z2)


def fb_kernel(x_ref, g_ref, w1_hbm, w2_hbm, y_ref, dx_ref, hall, gall, zall,
              bufa, bufb, dg, act, hin, hout, gin, gout, tmp, hbuf, zb0, zb1, zb2,
              wsem, tsem, hsem, zsem, xs, xr, gs, gr, fs, fr, bs, br, ys, yr, ds, dr, loc, ags, agr, *, ns):
    p = lax.axis_index("stage")
    q = lax.axis_index("inner")
    z, y = q // 4, q % 4
    d, f = bufa.shape
    ck = hin.shape[1]
    nmb = ns // 2
    sub = ck // nmb
    hf = ck // 2

    def at_stage(s):
        return {"data": 0, "inner": q, "stage": s}

    def at_plane(zz, yy):
        return {"data": 0, "inner": zz * 4 + yy, "stage": p}

    def rc(src, dst, ss, rs, dev):
        return pltpu.make_async_remote_copy(src_ref=src, dst_ref=dst, send_sem=ss, recv_sem=rs, device_id=dev, device_id_type=MESH)

    cw1 = pltpu.make_async_copy(w1_hbm, bufa, wsem.at[0])
    cw2 = pltpu.make_async_copy(w2_hbm, bufb, wsem.at[1])
    cw1.start()
    cw2.start()

    bar = pltpu.get_barrier_semaphore()
    for k in range(1, ns):
        pl.semaphore_signal(bar, inc=1, device_id=at_stage(lax.rem(p + k, ns)), device_id_type=MESH)
    for k in (1, 2, 3):
        pl.semaphore_signal(bar, inc=1, device_id=at_plane(lax.rem(z + k, 4), y), device_id_type=MESH)
        pl.semaphore_signal(bar, inc=1, device_id=at_plane(z, lax.rem(y + k, 4)), device_id_type=MESH)
    pl.semaphore_wait(bar, ns - 1 + 6)

    def mine(buf):
        return buf.at[p // nmb, pl.ds(pl.multiple_of(lax.rem(p, nmb) * sub, sub), sub)]

    def gather_x(s):
        return rc(x_ref, hin.at[s // nmb, pl.ds(pl.multiple_of(lax.rem(s, nmb) * sub, sub), sub)], xs, xr.at[s], at_stage(0))

    def gather_g(s):
        return rc(g_ref, gin.at[s // nmb, pl.ds(pl.multiple_of(lax.rem(s, nmb) * sub, sub), sub)], gs, gr.at[s], at_stage(ns - 1))

    @pl.when(p > 0)
    def _():
        gather_x(p).start()

    @pl.when(p < ns - 1)
    def _():
        gather_g(p).start()

    @pl.when(p == 0)
    def _():
        hin[0, :sub] = x_ref[...]

    @pl.when(p == ns - 1)
    def _():
        gin[1, ck - sub:] = g_ref[...]

    def hop_f(c):
        return rc(hout.at[c], hin.at[c], fs.at[c], fr.at[c], at_stage(lax.rem(p + 1, ns)))

    def hop_b(c):
        return rc(gout.at[c], gin.at[c], bs.at[c], br.at[c], at_stage(lax.rem(p + ns - 1, ns)))

    def put_y(c, m):
        return rc(hout.at[c, pl.ds(m * sub, sub)], y_ref, ys.at[c * nmb + m], yr, at_stage(c * nmb + m))

    def put_dx(c, m):
        return rc(gout.at[c, pl.ds(m * sub, sub)], dx_ref, ds.at[c * nmb + m], dr, at_stage(c * nmb + m))

    def blk(out, c, zz, yy):
        return out.at[zz, yy, c]

    def line(out, c, zz, yy):
        return out.at[:, yy, c] if c == 0 else out.at[zz, :, c]

    def half(ref, up, lead):
        rows = pl.ds(0, hf) if up else pl.ds(hf, hf)
        return ref.at[:, rows] if lead else ref.at[rows]

    def shift(c, first, k):
        along_z = (c == 0) == first
        return (lax.rem(z + k + 4, 4), y) if along_z else (z, lax.rem(y + k + 4, 4))

    def ag(buf, out, a, c, step, up):
        first = step in (0, 1)
        sgn = 1 if up else -1
        to = at_plane(*shift(c, first, sgn))
        j = (a * 2 + c) * 8 + step * 2 + (0 if up else 1)
        if step == 0:
            src, dst = buf.at[c], blk(out, c, z, y)
        elif step == 1:
            src = dst = half(blk(out, c, *shift(c, True, -sgn)), up, False)
        elif step == 2:
            src = dst = line(out, c, z, y)
        else:
            src = dst = half(line(out, c, *shift(c, False, -sgn)), up, True)
        return rc(src, dst, ags.at[j], agr.at[j], to)

    def own(buf, out, a, c):
        return pltpu.make_async_copy(buf.at[c], out.at[z, y, c], loc.at[a * 2 + c])

    def ag_start(buf, out, a, c, step):
        for up in (True, False):
            ag(buf, out, a, c, step, up).start()

    def ag_wait(buf, out, a, c, step):
        for up in (True, False):
            ag(buf, out, a, c, step, up).wait()

    H, G = (hin, hall, 0), (gin, gall, 1)
    last = ns - 1

    def ag_go(who, step):
        for c in (0, 1):
            ag_wait(*who, c, step - 1)
            ag_start(*who, c, step)

    def ag_end(who):
        for c in (0, 1):
            ag_wait(*who, c, 3)

    def ag_in(who, c):
        for cc in (0, 1):
            @pl.when(c == cc)
            def _():
                own(*who, cc).start()
                ag_start(*who, cc, 0)

    def ag_in_end(who):
        for c in (0, 1):
            own(*who, c).wait()
        ag_go(who, 1)

    def up(c, src, k):
        for j in range(0, d, 512):
            u = jnp.dot(act[k], bufb[:, j:j + 512], preferred_element_type=F32)
            hout[c, :, j:j + 512] = (src[:, j:j + 512].astype(F32) + u).astype(BF)

    def rows_of(c, r, n):
        return pl.ds(pl.multiple_of(c * ck + r, n), n)

    def fwd(c):
        h = hin.at[c]
        for j in range(0, f, 512):
            zz = jnp.dot(h[...], bufa[:, j:j + 512], preferred_element_type=F32)
            for r in range(0, ck, 32):
                a_, d_ = gelu_parts(zz[r:r + 32])
                act[0, r:r + 32, j:j + 512] = a_.astype(BF)
                dg[rows_of(c, r, 32), j:j + 512] = d_

        @pl.when(c == 0)
        def _():
            cw2.wait()
        up(c, h, 0)

    def bwd(c):
        g = gin.at[c]
        for j in range(0, f, 512):
            da = jnp.dot(g[...], bufa[:, j:j + 512], preferred_element_type=F32)
            for r in range(0, ck, 32):
                act[0, r:r + 32, j:j + 512] = (da[r:r + 32] * dg[rows_of(c, r, 32), j:j + 512]).astype(BF)
        for j in range(0, d, 512):
            u = jnp.dot(act[0], bufb[:, j:j + 512], preferred_element_type=F32)
            gout[c, :, j:j + 512] = (g[:, j:j + 512].astype(F32) + u).astype(BF)

    def turn(c):
        h, g = hin.at[c], gin.at[c]
        for j in range(0, f, 512):
            zz = jnp.dot(h[...], bufa[:, j:j + 512], preferred_element_type=F32)
            for r in range(0, ck, 32):
                a_, d_ = gelu_parts(zz[r:r + 32])
                act[c, r:r + 32, j:j + 512] = a_.astype(BF)
                act[2, r:r + 32, j:j + 512] = (dg[rows_of(c, r, 32), j:j + 512] * d_).astype(BF)
        for j in range(0, d, 512):
            u = lax.dot_general(act[2], bufa[j:j + 512, :], NT, preferred_element_type=F32)
            gout[c, :, j:j + 512] = (g[:, j:j + 512].astype(F32) + u).astype(BF)

    cw1.wait()

    @pl.when(p < last)
    def _():
        @pl.loop(0, 2)
        def _(c):
            @pl.when(p == 0)
            def _():
                for m in range(nmb):
                    @pl.when(c * nmb + m > 0)
                    def _():
                        gather_x(c * nmb + m).wait_recv()

            @pl.when(p > 0)
            def _():
                hop_f(c).wait_recv()
            ag_in(H, c)
            fwd(c)
            hop_f(c).start()
        ag_in_end(H)

    @pl.when(p == last)
    def _():
        cw2.wait()
        for s in range(last):
            gather_g(s).wait_recv()
        for c in (0, 1):
            own(*G, c).start()
            ag_start(*G, c, 0)

        @pl.loop(0, 2)
        def _(c):
            for j in range(0, f, 512):
                dg[rows_of(c, 0, ck), j:j + 512] = lax.dot_general(gin[c], bufb[j:j + 512, :], NT, preferred_element_type=F32)
        for c in (0, 1):
            own(*G, c).wait()
        for step in (1, 2, 3):
            ag_go(G, step)

        @pl.loop(0, 2)
        def _(c):
            hop_f(c).wait_recv()
            ag_in(H, c)
            turn(c)
            hop_b(c).start()

        @pl.loop(0, 2)
        def _(c):
            up(c, hin.at[c], c)
            for m in range(nmb):
                @pl.when(c * nmb + m < last)
                def _():
                    put_y(c, m).start()
        pltpu.make_async_copy(hout.at[1, pl.ds(ck - sub, sub)], y_ref, yr).start()
        ag_in_end(H)
        ag_go(H, 2)

    @pl.when(p < last - 1)
    def _():
        ag_go(H, 2)

    nt = 512

    def tload(i, s):
        return pltpu.make_async_copy(w1_hbm.at[:, pl.ds(pl.multiple_of(i * nt, nt), nt)], tmp.at[s], tsem.at[s])
    tload(0, 0).start()

    @pl.loop(0, f // nt)
    def _(i):
        for r in range(0, nt, 128):
            rows = pl.ds(pl.multiple_of(i * nt + r, 128), 128)
            bufa[:, rows] = bufb[rows, :].T

    @pl.loop(0, f // nt)
    def _(i):
        s = lax.rem(i, 2)

        @pl.when(i + 1 < f // nt)
        def _():
            tload(i + 1, 1 - s).start()
        tload(i, s).wait()
        for r in range(0, nt, 128):
            bufb[pl.ds(pl.multiple_of(i * nt + r, 128), 128), :] = tmp[s, :, r:r + 128].T

    @pl.when(p == last - 1)
    def _():
        ag_go(H, 2)

    nf = zall.shape[0] // 512
    zb = (zb0, zb1, zb2)

    def line_of(t):
        c = jnp.where((t == 1) | (t == 4) | (t == 5) | (t == 7), 1, 0)
        off = jnp.where(t < 2, 0, jnp.where(t >= 6, 2, jnp.where(lax.rem(t, 2) == 0, 1, 3)))
        return c, lax.rem(jnp.where(c == 0, y, z) + off, 4)

    def hload(t, k):
        _, l = line_of(t)
        s = lax.rem(t, 2)
        src = hall.at[:, l, 0] if k == 0 else hall.at[l, :, 1]
        return pltpu.make_async_copy(src, hbuf.at[s], hsem.at[s])

    def hstart(t):
        for k in (0, 1):
            @pl.when(line_of(t)[0] == k)
            def _():
                hload(t, k).start()

    def zput(t, j, u):
        c, l = line_of(t)
        rows = pl.ds(pl.multiple_of(j * 512, 512), 512)
        cols = pl.ds(pl.multiple_of((c * 4 + l) * 512, 512), 512)
        return pltpu.make_async_copy(zb[u], zall.at[rows, cols], zsem.at[u])

    def zwork(t0, t1):
        hstart(t0)

        @pl.loop(t0, t1)
        def _(t):
            hload(t, 0).wait()

            @pl.when(t + 1 < t1)
            def _():
                hstart(t + 1)

            @pl.loop(0, nf // 3)
            def _(k):
                for u in range(3):
                    j = 3 * k + u

                    @pl.when((t > t0) | (k > 0))
                    def _():
                        zput(t, j, u).wait()
                    rows = pl.ds(pl.multiple_of(j * 512, 512), 512)
                    hc = hbuf[lax.rem(t, 2)].reshape(512, d)
                    zb[u][...] = lax.dot_general(bufb[rows, :], hc, NT, preferred_element_type=F32)
                    zput(t, j, u).start()
        for u in range(3):
            zput(t0, u, u).wait()

    pre = jnp.where(p < 2, 8, jnp.where(p < 5, 10 - 2 * p, 0))

    @pl.loop(0, 6)
    def _(ph):
        @pl.when((ph == 1) & (p < 4))
        def _():
            ag_go(H, 3)

        @pl.when((ph == 2) & (p < 2))
        def _():
            ag_end(H)

        @pl.when((ph == 3) & (p < last))
        def _():
            @pl.loop(0, 2)
            def _(c):
                hop_b(c).wait_recv()
                ag_in(G, c)
                bwd(c)

                @pl.when(p > 0)
                def _():
                    hop_b(c).start()

                @pl.when(p == 0)
                def _():
                    for m in range(nmb):
                        @pl.when(c * nmb + m > 0)
                        def _():
                            put_dx(c, m).start()

            @pl.when(p == 0)
            def _():
                pltpu.make_async_copy(gout.at[0, pl.ds(0, sub)], dx_ref, dr).start()
            ag_in_end(G)

        @pl.when((ph == 4) & (p >= 4))
        def _():
            ag_go(H, 3)

        @pl.when((ph == 4) & (p < last))
        def _():
            ag_go(G, 2)

        @pl.when((ph == 5) & (p >= 2))
        def _():
            ag_end(H)

        @pl.when((ph == 5) & (p < last))
        def _():
            ag_go(G, 3)

        k = lax.rem(ph, 3)
        edge = jnp.where(k == 0, 0, jnp.where(k == 1, 2, 6))
        edge1 = jnp.where(k == 0, 2, jnp.where(k == 1, 6, 8))
        lo = jnp.where(ph < 3, edge, jnp.maximum(edge, pre))
        hi = jnp.where(ph < 3, jnp.minimum(edge1, pre), edge1)

        @pl.when(lo < hi)
        def _():
            zwork(lo, hi)
    ag_end(G)

    @pl.when(p > 0)
    def _():
        gather_x(p).wait_send()
        hop_b(0).wait_send()
        hop_b(1).wait_send()
        put_dx(0, 0).wait_recv()

    @pl.when(p == 0)
    def _():
        for s in range(1, ns):
            put_dx(s // nmb, s % nmb).wait_send()
        pltpu.make_async_copy(gout.at[0, pl.ds(0, sub)], dx_ref, dr).wait()

    @pl.when(p < ns - 1)
    def _():
        gather_g(p).wait_send()
        hop_f(0).wait_send()
        hop_f(1).wait_send()
        put_y(0, 0).wait_recv()

    @pl.when(p == ns - 1)
    def _():
        for s in range(ns - 1):
            put_y(s // nmb, s % nmb).wait_send()
        pltpu.make_async_copy(hout.at[1, pl.ds(ck - sub, sub)], y_ref, yr).wait()


def fb(x, g, w1, w2, nz, ns=8):
    b, d = x.shape
    f = w1.shape[1]
    ck = b * ns // 2
    dma = pltpu.SemaphoreType.DMA
    vm = pl.BlockSpec(memory_space=pltpu.VMEM)
    hbm = pl.BlockSpec(memory_space=pl.ANY)
    allt = jax.ShapeDtypeStruct((4, 4, 2, ck, d), BF)
    y, dx, h, gg, z = pl.pallas_call(
        functools.partial(fb_kernel, ns=ns),
        in_specs=[vm, vm, hbm, hbm],
        out_specs=[hbm] * 5,
        out_shape=[jax.ShapeDtypeStruct((b, d), BF)] * 2 + [allt] * 2 + [jax.ShapeDtypeStruct((nz, 32 * ck), F32)],
        scratch_shapes=[
            pltpu.VMEM((d, f), BF), pltpu.VMEM((f, d), BF), pltpu.VMEM((2 * ck, f), F32), pltpu.VMEM((3, ck, f), BF),
            pltpu.VMEM((2, ck, d), BF), pltpu.VMEM((2, ck, d), BF), pltpu.VMEM((2, ck, d), BF), pltpu.VMEM((2, ck, d), BF),
            pltpu.VMEM((2, d, 512), BF), pltpu.VMEM((2, 4, ck, d), BF), pltpu.VMEM((512, 512), F32), pltpu.VMEM((512, 512), F32), pltpu.VMEM((512, 512), F32),
            dma((2,)), dma((2,)), dma((2,)), dma((3,)), dma, dma((ns,)), dma, dma((ns,)), dma((2,)), dma((2,)), dma((2,)), dma((2,)),
            dma((ns,)), dma, dma((ns,)), dma, dma((4,)), dma((32,)), dma((32,)),
        ],
        compiler_params=pltpu.CompilerParams(vmem_limit_bytes=VMEM_BYTES, collective_id=0, has_side_effects=True),
        name="fb",
    )(x, g, w1, w2)
    return y, dx, h, gg, z


def wgrad_kernel(z_hbm, w2_ref, h_hbm, g_hbm, dw1_ref, dw2_ref, h_ref, g_ref, at, dzt, z0, z1, d0, d1, hsem, zsem):
    b = pl.program_id(0)
    nb = pl.num_programs(0)
    n, d = h_ref.shape[0], h_ref.shape[3]
    f, tc = d0.shape
    t = n * tc
    half = t // 2
    zs, ds = (z0, z1), (d0, d1)

    def zget(blk, i):
        rows = pl.ds(pl.multiple_of(blk * f, f), f)
        return pltpu.make_async_copy(z_hbm.at[rows, pl.ds(i * half, half)], zs[i], zsem.at[i])

    def get(src, dst, i, k):
        return pltpu.make_async_copy(src.at[:, i, 0] if i < 4 else src.at[i - 4, :, 1], dst.at[i], hsem.at[k, i])

    @pl.when(b == 0)
    def _():
        for i in range(n):
            get(g_hbm, g_ref, i, 0).start()
        zget(0, 0).start()
        zget(0, 1).start()
        for i in range(n):
            get(h_hbm, h_ref, i, 1).start()
        for i in range(n):
            get(g_hbm, g_ref, i, 0).wait()

    def dots(i):
        ds[i % 2][...] = lax.dot_general(w2_ref[...], g_ref[i].reshape(tc, d), NT, preferred_element_type=F32)

    def elem(i):
        cols = pl.ds(i * tc, tc)
        off = (i * tc) % half
        for r in range(0, f, 32):
            a, da = gelu_parts(zs[i * tc // half][r:r + 32, off:off + tc])
            at[r:r + 32, cols] = a.astype(BF)
            dzt[r:r + 32, cols] = (ds[i % 2][r:r + 32, :] * da).astype(BF)

    zget(b, 0).wait()
    dots(0)
    for i in range(1, n // 2 + 1):
        dots(i)
        elem(i - 1)
    zget(b, 1).wait()

    @pl.when(b + 1 < nb)
    def _():
        zget(b + 1, 0).start()

    @pl.when(b == 0)
    def _():
        for i in range(n):
            get(h_hbm, h_ref, i, 1).wait()
    for i in range(n // 2 + 1, n):
        dots(i)
        elem(i - 1)
    elem(n - 1)
    for j in range(0, d, 512):
        cols = pl.ds(j, 512)
        p1 = jnp.dot(dzt[...], h_ref[:, :, :, cols].reshape(t, 512), preferred_element_type=F32)
        for r in range(0, 512, 128):
            dw1_ref[pl.ds(j + r, 128), :] = p1[:, r:r + 128].T
        dw2_ref[:, cols] = jnp.dot(at[...], g_ref[:, :, :, cols].reshape(t, 512), preferred_element_type=F32)

    @pl.when(b + 1 < nb)
    def _():
        zget(b + 1, 1).start()


def wgrad(z, w2, h, g, f=512, tc=512):
    ff, d = w2.shape
    t = z.shape[1]
    nb = z.shape[0] // f
    kept = pltpu.VMEM((t // tc, 4, tc // 4, d), BF)
    hbm = pl.BlockSpec(memory_space=pl.ANY)
    dma = pltpu.SemaphoreType.DMA
    return pl.pallas_call(
        wgrad_kernel,
        grid=(nb,),
        in_specs=[hbm, pl.BlockSpec((f, d), lambda i: (i, 0)), hbm, hbm],
        out_specs=[pl.BlockSpec((d, f), lambda i: (0, i)), pl.BlockSpec((f, d), lambda i: (i, 0))],
        out_shape=[jax.ShapeDtypeStruct((d, ff), F32), jax.ShapeDtypeStruct((ff, d), F32)],
        scratch_shapes=[kept] * 2 + [pltpu.VMEM((f, t), BF)] * 2 + [pltpu.VMEM((f, t // 2), F32)] * 2 + [pltpu.VMEM((f, tc), F32)] * 2
        + [dma((2, t // tc)), dma((2,))],
        compiler_params=pltpu.CompilerParams(vmem_limit_bytes=VMEM_BYTES, dimension_semantics=("arbitrary",)),
        cost_estimate=pl.CostEstimate(flops=6 * t * d * ff, bytes_accessed=10 * d * ff + 4 * t * d + 4 * t * ff, transcendentals=t * ff),
        name="wgrad",
    )(z, w2, h, g)


def share_kernel(w1t, w2, h_hbm, g_hbm, s1, s2, h_ref, g_ref, at, dzt, hsem, gsem, *, tc):
    t = h_ref.shape[0]
    n = t // tc

    def part(src, dst, sem, i):
        rows = pl.ds(i * tc if isinstance(i, int) else pl.multiple_of(i * tc, tc), tc)
        return pltpu.make_async_copy(src.at[rows], dst.at[rows], sem.at[i])
    for i in range(n):
        part(h_hbm, h_ref, hsem, i).start()
        part(g_hbm, g_ref, gsem, i).start()

    @pl.loop(0, n)
    def _(i):
        rows = pl.ds(pl.multiple_of(i * tc, tc), tc)
        part(h_hbm, h_ref, hsem, i).wait()
        part(g_hbm, g_ref, gsem, i).wait()
        z = lax.dot_general(w1t[...], h_ref[rows, :], NT, preferred_element_type=F32)
        da = lax.dot_general(w2[...], g_ref[rows, :], NT, preferred_element_type=F32)
        a, dg = gelu_parts(z)
        at[:, rows] = a.astype(BF)
        dzt[:, rows] = (da * dg).astype(BF)

    @pl.loop(0, h_ref.shape[1] // 512)
    def _(j):
        cols = pl.ds(pl.multiple_of(j * 512, 512), 512)
        s1[:, cols] = jnp.dot(dzt[...], h_ref[:, cols], preferred_element_type=F32)
        s2[:, cols] = jnp.dot(at[...], g_ref[:, cols], preferred_element_type=F32)


def share(w1t, w2, h, g, tc=1024):
    fs, d = w2.shape
    t = h.shape[0]
    vm = pl.BlockSpec(memory_space=pltpu.VMEM)
    hbm = pl.BlockSpec(memory_space=pl.ANY)
    dma = pltpu.SemaphoreType.DMA
    return pl.pallas_call(
        functools.partial(share_kernel, tc=tc),
        in_specs=[vm, vm, hbm, hbm],
        out_specs=[vm, vm],
        out_shape=[jax.ShapeDtypeStruct((fs, d), F32)] * 2,
        scratch_shapes=[pltpu.VMEM((t, d), BF)] * 2 + [pltpu.VMEM((fs, t), BF)] * 2 + [dma((t // tc,)), dma((t // tc,))],
        compiler_params=pltpu.CompilerParams(vmem_limit_bytes=VMEM_BYTES),
        cost_estimate=pl.CostEstimate(flops=16 * t * d * fs, bytes_accessed=4 * t * d, transcendentals=t * fs),
        name="share",
    )(w1t, w2, h, g)


def finish_kernel(s1, s2, dw1_in, dw2_in, dw1, dw2):
    del dw1_in, dw2_in
    for r in range(0, s1.shape[1], 256):
        dw1[pl.ds(r, 256), :] = s1[:, r:r + 256].T
    dw2[...] = s2[...]


def finish(s1, s2, dw1, dw2, first, f=512):
    n, d = s1.shape
    hbm = pl.BlockSpec(memory_space=pl.ANY)
    row = pl.BlockSpec((f, d), lambda i: (i, 0))
    return pl.pallas_call(
        finish_kernel,
        grid=(n // f,),
        in_specs=[row, row, hbm, hbm],
        out_specs=[pl.BlockSpec((d, f), lambda i: (0, first + i)), pl.BlockSpec((f, d), lambda i: (first + i, 0))],
        out_shape=[jax.ShapeDtypeStruct(dw1.shape, F32), jax.ShapeDtypeStruct(dw2.shape, F32)],
        input_output_aliases={2: 0, 3: 1},
        compiler_params=pltpu.CompilerParams(vmem_limit_bytes=VMEM_BYTES, dimension_semantics=("arbitrary",)),
        cost_estimate=pl.CostEstimate(flops=n * d, bytes_accessed=16 * n * d, transcendentals=0),
        name="finish",
    )(s1, s2, dw1, dw2)


def solution(mesh):
    def body(x, g, w1, w2):
        w1, w2 = w1[0, 0], w2[0, 0]
        ff, d = w2.shape
        nz = NB * 512
        fs = (ff - nz) // 16
        at = nz + lax.axis_index("inner") * fs
        w1t = lax.dynamic_slice(w1, (0, at), (d, fs)).T
        w2s = lax.dynamic_slice(w2, (at, 0), (fs, d))
        y, dx, h, gg, z = fb(x[0], g[0], w1, w2, nz)
        s1, s2 = share(w1t, w2s, h.reshape(-1, d), gg.reshape(-1, d))
        s1 = lax.all_gather(s1, "inner", axis=0, tiled=True)
        s2 = lax.all_gather(s2, "inner", axis=0, tiled=True)
        dw1, dw2 = wgrad(z, w2, h, gg)
        dw1, dw2 = finish(s1, s2, dw1, dw2, NB)
        return y[None], dx[None], dw1[None, None], dw2[None, None]

    tok = P(("data", "stage"), "inner", None)
    wsp = P(None, "stage", None, None)
    dsp = P("data", "stage", None, None)
    return jax.shard_map(body, mesh=mesh, in_specs=(tok, tok, wsp, wsp), out_specs=(tok, tok, dsp, dsp), check_vma=False)
```

```python
import functools

import jax
import jax.numpy as jnp
from jax import lax
from jax.experimental import pallas as pl
from jax.experimental.pallas import tpu as pltpu
from jax.sharding import PartitionSpec as P

MESH = pl.DeviceIdType.MESH
BF, F32 = jnp.bfloat16, jnp.float32
NT = (((1,), (1,)), ((), ()))
C0 = 0.7978845608028654
C1 = 0.044715
VMEM_BYTES = 67043328
NB = 9
BLK = 512


def gelu_parts(z):
    z2 = z * z
    t = jnp.tanh(z * (C0 + (C0 * C1) * z2))
    cdf = 0.5 + 0.5 * t
    return z * cdf, cdf + (0.5 * z) * (1.0 - t * t) * (C0 + (3.0 * C0 * C1) * z2)


def fb_kernel(x_ref, g_ref, w1_hbm, w2_hbm, y_ref, dx_ref, hall, gall, zall,
              bufa, bufb, dg, act, hin, hout, gin, gout, tmp, hbuf, zb0, zb1, zb2,
              wsem, tsem, hsem, zsem, xs, xr, gs, gr, fs, fr, bs, br, ys, yr, ds, dr, loc, ags, agr, *, ns):
    p = lax.axis_index("stage")
    q = lax.axis_index("inner")
    z, y = q // 4, q % 4
    d, f = bufa.shape
    ck = hin.shape[1]
    nmb = ns // 2
    sub = ck // nmb
    hf = ck // 2

    def at_stage(s):
        return {"inner": q, "stage": s}

    def at_plane(zz, yy):
        return {"inner": zz * 4 + yy, "stage": p}

    def rc(src, dst, ss, rs, dev):
        return pltpu.make_async_remote_copy(src_ref=src, dst_ref=dst, send_sem=ss, recv_sem=rs, device_id=dev, device_id_type=MESH)

    cw1 = pltpu.make_async_copy(w1_hbm, bufa, wsem.at[0])
    cw2 = pltpu.make_async_copy(w2_hbm, bufb, wsem.at[1])
    cw1.start()
    cw2.start()

    bar = pltpu.get_barrier_semaphore()
    for k in range(1, ns):
        pl.semaphore_signal(bar, inc=1, device_id=at_stage(lax.rem(p + k, ns)), device_id_type=MESH)
    for k in (1, 2, 3):
        pl.semaphore_signal(bar, inc=1, device_id=at_plane(lax.rem(z + k, 4), y), device_id_type=MESH)
        pl.semaphore_signal(bar, inc=1, device_id=at_plane(z, lax.rem(y + k, 4)), device_id_type=MESH)
    pl.semaphore_wait(bar, ns - 1 + 6)

    def mine(buf):
        return buf.at[p // nmb, pl.ds(pl.multiple_of(lax.rem(p, nmb) * sub, sub), sub)]

    def gather_x(s):
        return rc(x_ref, hin.at[s // nmb, pl.ds(pl.multiple_of(lax.rem(s, nmb) * sub, sub), sub)], xs, xr.at[s], at_stage(0))

    def gather_g(s):
        return rc(g_ref, gin.at[s // nmb, pl.ds(pl.multiple_of(lax.rem(s, nmb) * sub, sub), sub)], gs, gr.at[s], at_stage(ns - 1))

    @pl.when(p > 0)
    def _():
        gather_x(p).start()

    @pl.when(p < ns - 1)
    def _():
        gather_g(p).start()

    @pl.when(p == 0)
    def _():
        hin[0, :sub] = x_ref[...]

    @pl.when(p == ns - 1)
    def _():
        gin[1, ck - sub:] = g_ref[...]

    def hop_f(c, k):
        cols = pl.ds(k * BLK, BLK)
        return rc(hout.at[c, :, cols], hin.at[c, :, cols], fs.at[c, k], fr.at[c, k], at_stage(lax.rem(p + 1, ns)))

    def hop_b(c, k):
        cols = pl.ds(k * BLK, BLK)
        return rc(gout.at[c, :, cols], gin.at[c, :, cols], bs.at[c, k], br.at[c, k], at_stage(lax.rem(p + ns - 1, ns)))

    nk = d // BLK

    def put_y(c, m):
        return rc(hout.at[c, pl.ds(m * sub, sub)], y_ref, ys.at[c * nmb + m], yr, at_stage(c * nmb + m))

    def put_dx(c, m):
        return rc(gout.at[c, pl.ds(m * sub, sub)], dx_ref, ds.at[c * nmb + m], dr, at_stage(c * nmb + m))

    def blk(out, c, zz, yy):
        return out.at[zz, yy, c]

    def line(out, c, zz, yy):
        return out.at[:, yy, c] if c == 0 else out.at[zz, :, c]

    def half(ref, up, lead):
        rows = pl.ds(0, hf) if up else pl.ds(hf, hf)
        return ref.at[:, rows] if lead else ref.at[rows]

    def shift(c, first, k):
        along_z = (c == 0) == first
        return (lax.rem(z + k + 4, 4), y) if along_z else (z, lax.rem(y + k + 4, 4))

    def ag(buf, out, a, c, step, up):
        first = step in (0, 1)
        sgn = 1 if up else -1
        to = at_plane(*shift(c, first, sgn))
        j = (a * 2 + c) * 8 + step * 2 + (0 if up else 1)
        if step == 0:
            src, dst = buf.at[c], blk(out, c, z, y)
        elif step == 1:
            src = dst = half(blk(out, c, *shift(c, True, -sgn)), up, False)
        elif step == 2:
            src = dst = line(out, c, z, y)
        else:
            src = dst = half(line(out, c, *shift(c, False, -sgn)), up, True)
        return rc(src, dst, ags.at[j], agr.at[j], to)

    def own(buf, out, a, c):
        return pltpu.make_async_copy(buf.at[c], out.at[z, y, c], loc.at[a * 2 + c])

    def ag_start(buf, out, a, c, step):
        for up in (True, False):
            ag(buf, out, a, c, step, up).start()

    def ag_wait(buf, out, a, c, step):
        for up in (True, False):
            ag(buf, out, a, c, step, up).wait()

    H, G = (hin, hall, 0), (gin, gall, 1)
    last = ns - 1

    def ag_go(who, step):
        for c in (0, 1):
            ag_wait(*who, c, step - 1)
            ag_start(*who, c, step)

    def ag_end(who):
        for c in (0, 1):
            ag_wait(*who, c, 3)

    def ag_in(who, c):
        for cc in (0, 1):
            @pl.when(c == cc)
            def _():
                own(*who, cc).start()
                ag_start(*who, cc, 0)

    def ag_in_end(who):
        for c in (0, 1):
            own(*who, c).wait()
        ag_go(who, 1)


    def rows_of(c, r, n):
        return pl.ds(pl.multiple_of(c * ck + r, n), n)

    def fwd(c):
        h = hin.at[c]
        for j in range(0, f, BLK):
            zz = jnp.dot(h[...], bufa[:, j:j + BLK], preferred_element_type=F32)
            for r in range(0, ck, 32):
                a_, d_ = gelu_parts(zz[r:r + 32])
                act[0, r:r + 32, j:j + BLK] = a_.astype(BF)
                dg[rows_of(c, r, 32), j:j + BLK] = d_

        @pl.when(c == 0)
        def _():
            cw2.wait()
        for k in range(nk):
            cols = pl.ds(k * BLK, BLK)
            u = jnp.dot(act[0], bufb[:, cols], preferred_element_type=F32)
            hout[c, :, cols] = (h[:, cols].astype(F32) + u).astype(BF)
            hop_f(c, k).start()

    def bwd(c):
        g = gin.at[c]
        for j in range(0, f, BLK):
            da = jnp.dot(g[...], bufa[:, j:j + BLK], preferred_element_type=F32)
            for r in range(0, ck, 32):
                act[0, r:r + 32, j:j + BLK] = (da[r:r + 32] * dg[rows_of(c, r, 32), j:j + BLK]).astype(BF)
        for k in range(nk):
            cols = pl.ds(k * BLK, BLK)
            u = jnp.dot(act[0], bufb[:, cols], preferred_element_type=F32)
            gout[c, :, cols] = (g[:, cols].astype(F32) + u).astype(BF)

            @pl.when(p > 0)
            def _():
                hop_b(c, k).start()

    def turn(c):
        h, g = hin.at[c], gin.at[c]
        for j in range(0, f, BLK):
            zz = jnp.dot(h[...], bufa[:, j:j + BLK], preferred_element_type=F32)
            for r in range(0, ck, 32):
                a_, d_ = gelu_parts(zz[r:r + 32])
                act[c, r:r + 32, j:j + BLK] = a_.astype(BF)
                act[2, r:r + 32, j:j + BLK] = (dg[rows_of(c, r, 32), j:j + BLK] * d_).astype(BF)
        for k in range(nk):
            cols = pl.ds(k * BLK, BLK)
            u = lax.dot_general(act[2], bufa[cols, :], NT, preferred_element_type=F32)
            gout[c, :, cols] = (g[:, cols].astype(F32) + u).astype(BF)
            hop_b(c, k).start()

    cw1.wait()

    @pl.when(p < last)
    def _():
        @pl.loop(0, 2)
        def _(c):
            @pl.when(p == 0)
            def _():
                for m in range(nmb):
                    @pl.when(c * nmb + m > 0)
                    def _():
                        gather_x(c * nmb + m).wait_recv()

            @pl.when(p > 0)
            def _():
                for k in range(nk):
                    hop_f(c, k).wait_recv()
            ag_in(H, c)
            fwd(c)
        ag_in_end(H)

    @pl.when(p == last)
    def _():
        cw2.wait()
        for s in range(last):
            gather_g(s).wait_recv()
        for c in (0, 1):
            own(*G, c).start()
            ag_start(*G, c, 0)

        @pl.loop(0, 2)
        def _(c):
            @pl.loop(0, f // 1024)
            def _(i):
                for r in (0, BLK):
                    js = pl.ds(pl.multiple_of(i * 1024 + r, BLK), BLK)
                    dg[rows_of(c, 0, ck), js] = lax.dot_general(gin[c], bufb[js, :], NT, preferred_element_type=F32)
        for c in (0, 1):
            own(*G, c).wait()
        for step in (1, 2, 3):
            ag_go(G, step)

        @pl.loop(0, 2)
        def _(c):
            for k in range(nk):
                hop_f(c, k).wait_recv()
            ag_in(H, c)
            turn(c)

        @pl.loop(0, 2)
        def _(c):
            @pl.loop(0, nk)
            def _(k):
                cols = pl.ds(pl.multiple_of(k * BLK, BLK), BLK)
                u = jnp.dot(act[c], bufb[:, cols], preferred_element_type=F32)
                hout[c, :, cols] = (hin[c, :, cols].astype(F32) + u).astype(BF)
            for m in range(nmb):
                @pl.when(c * nmb + m < last)
                def _():
                    put_y(c, m).start()
        pltpu.make_async_copy(hout.at[1, pl.ds(ck - sub, sub)], y_ref, yr).start()
        ag_in_end(H)
        ag_go(H, 2)

    @pl.when(p < last - 1)
    def _():
        ag_go(H, 2)

    nt = BLK

    def tload(i, s):
        return pltpu.make_async_copy(w1_hbm.at[:, pl.ds(pl.multiple_of(i * nt, nt), nt)], tmp.at[s], tsem.at[s])
    tload(0, 0).start()

    @pl.loop(0, f // nt)
    def _(i):
        for r in range(0, nt, 128):
            rows = pl.ds(pl.multiple_of(i * nt + r, 128), 128)
            bufa[:, rows] = bufb[rows, :].T

    @pl.loop(0, f // nt)
    def _(i):
        s = lax.rem(i, 2)

        @pl.when(i + 1 < f // nt)
        def _():
            tload(i + 1, 1 - s).start()
        tload(i, s).wait()
        for r in range(0, nt, 128):
            bufb[pl.ds(pl.multiple_of(i * nt + r, 128), 128), :] = tmp[s, :, r:r + 128].T

    @pl.when(p == last - 1)
    def _():
        ag_go(H, 2)

    nf = zall.shape[0] // BLK
    zb = (zb0, zb1, zb2)

    def line_of(t):
        c = jnp.where((t == 1) | (t == 4) | (t == 5) | (t == 7), 1, 0)
        off = jnp.where(t < 2, 0, jnp.where(t >= 6, 2, jnp.where(lax.rem(t, 2) == 0, 1, 3)))
        return c, lax.rem(jnp.where(c == 0, y, z) + off, 4)

    def hload(t, k):
        _, l = line_of(t)
        s = lax.rem(t, 2)
        src = hall.at[:, l, 0] if k == 0 else hall.at[l, :, 1]
        return pltpu.make_async_copy(src, hbuf.at[s], hsem.at[s])

    def hstart(t):
        for k in (0, 1):
            @pl.when(line_of(t)[0] == k)
            def _():
                hload(t, k).start()

    def zput(t, j, u):
        c, l = line_of(t)
        rows = pl.ds(pl.multiple_of(j * BLK, BLK), BLK)
        cols = pl.ds(pl.multiple_of((c * 4 + l) * BLK, BLK), BLK)
        return pltpu.make_async_copy(zb[u], zall.at[rows, cols], zsem.at[u])

    def zwork(t0, t1):
        hstart(t0)

        @pl.loop(t0, t1)
        def _(t):
            hload(t, 0).wait()

            @pl.when(t + 1 < t1)
            def _():
                hstart(t + 1)

            @pl.loop(0, nf // 3)
            def _(k):
                for u in range(3):
                    j = 3 * k + u

                    @pl.when((t > t0) | (k > 0))
                    def _():
                        zput(t, j, u).wait()
                    rows = pl.ds(pl.multiple_of(j * BLK, BLK), BLK)
                    hc = hbuf[lax.rem(t, 2)].reshape(BLK, d)
                    zb[u][...] = lax.dot_general(bufb[rows, :], hc, NT, preferred_element_type=F32)
                    zput(t, j, u).start()
        for u in range(3):
            zput(t0, u, u).wait()

    pre = jnp.where(p < 2, 8, jnp.where(p < 5, 10 - 2 * p, 0))

    @pl.loop(0, 6)
    def _(ph):
        @pl.when((ph == 1) & (p < 4))
        def _():
            ag_go(H, 3)

        @pl.when((ph == 2) & (p < 2))
        def _():
            ag_end(H)

        @pl.when((ph == 3) & (p < last))
        def _():
            @pl.loop(0, 2)
            def _(c):
                for k in range(nk):
                    hop_b(c, k).wait_recv()
                ag_in(G, c)
                bwd(c)

                @pl.when(p == 0)
                def _():
                    for m in range(nmb):
                        @pl.when(c * nmb + m > 0)
                        def _():
                            put_dx(c, m).start()

            @pl.when(p == 0)
            def _():
                pltpu.make_async_copy(gout.at[0, pl.ds(0, sub)], dx_ref, dr).start()
            ag_in_end(G)

        @pl.when((ph == 4) & (p >= 4))
        def _():
            ag_go(H, 3)

        @pl.when((ph == 4) & (p < last))
        def _():
            ag_go(G, 2)

        @pl.when((ph == 5) & (p >= 2))
        def _():
            ag_end(H)

        @pl.when((ph == 5) & (p < last))
        def _():
            ag_go(G, 3)

        k = lax.rem(ph, 3)
        edge = jnp.where(k == 0, 0, jnp.where(k == 1, 2, 6))
        edge1 = jnp.where(k == 0, 2, jnp.where(k == 1, 6, 8))
        lo = jnp.where(ph < 3, edge, jnp.maximum(edge, pre))
        hi = jnp.where(ph < 3, jnp.minimum(edge1, pre), edge1)

        @pl.when(lo < hi)
        def _():
            zwork(lo, hi)
    ag_end(G)

    @pl.when(p > 0)
    def _():
        gather_x(p).wait_send()
        for c in (0, 1):
            for k in range(nk):
                hop_b(c, k).wait_send()
        put_dx(0, 0).wait_recv()

    @pl.when(p == 0)
    def _():
        for s in range(1, ns):
            put_dx(s // nmb, s % nmb).wait_send()
        pltpu.make_async_copy(gout.at[0, pl.ds(0, sub)], dx_ref, dr).wait()

    @pl.when(p < ns - 1)
    def _():
        gather_g(p).wait_send()
        for c in (0, 1):
            for k in range(nk):
                hop_f(c, k).wait_send()
        put_y(0, 0).wait_recv()

    @pl.when(p == ns - 1)
    def _():
        for s in range(ns - 1):
            put_y(s // nmb, s % nmb).wait_send()
        pltpu.make_async_copy(hout.at[1, pl.ds(ck - sub, sub)], y_ref, yr).wait()


def fb(x, g, w1, w2, nz, ns=8):
    b, d = x.shape
    f = w1.shape[1]
    ck = b * ns // 2
    nk = d // BLK
    dma = pltpu.SemaphoreType.DMA
    vm = pl.BlockSpec(memory_space=pltpu.VMEM)
    hbm = pl.BlockSpec(memory_space=pl.ANY)
    allt = jax.ShapeDtypeStruct((4, 4, 2, ck, d), BF)
    y, dx, h, gg, z = pl.pallas_call(
        functools.partial(fb_kernel, ns=ns),
        in_specs=[vm, vm, hbm, hbm],
        out_specs=[hbm] * 5,
        out_shape=[jax.ShapeDtypeStruct((b, d), BF)] * 2 + [allt] * 2 + [jax.ShapeDtypeStruct((nz, 32 * ck), F32)],
        scratch_shapes=[pltpu.VMEM((d, f), BF), pltpu.VMEM((f, d), BF), pltpu.VMEM((2 * ck, f), F32), pltpu.VMEM((3, ck, f), BF)]
        + [pltpu.VMEM((2, ck, d), BF)] * 4
        + [pltpu.VMEM((2, d, BLK), BF), pltpu.VMEM((2, 4, ck, d), BF)]
        + [pltpu.VMEM((BLK, BLK), F32)] * 3
        + [dma((2,))] * 3
        + [dma((3,))]
        + [dma, dma((ns,))] * 2
        + [dma((2, nk))] * 4
        + [dma((ns,)), dma] * 2
        + [dma((4,)), dma((32,)), dma((32,))],
        compiler_params=pltpu.CompilerParams(vmem_limit_bytes=VMEM_BYTES, collective_id=0, has_side_effects=True),
        name="fb",
    )(x, g, w1, w2)
    return y, dx, h, gg, z


def wgrad_kernel(z_hbm, w2_ref, h_hbm, g_hbm, dw1_ref, dw2_ref, h_ref, g_ref, at, dzt, z0, z1, d0, d1, hsem, zsem):
    b = pl.program_id(0)
    nb = pl.num_programs(0)
    n, d = h_ref.shape[0], h_ref.shape[3]
    f, tc = d0.shape
    t = n * tc
    half = t // 2
    zs, ds = (z0, z1), (d0, d1)

    def zget(blk, i):
        rows = pl.ds(pl.multiple_of(blk * f, f), f)
        return pltpu.make_async_copy(z_hbm.at[rows, pl.ds(i * half, half)], zs[i], zsem.at[i])

    def get(src, dst, i, k):
        return pltpu.make_async_copy(src.at[:, i, 0] if i < 4 else src.at[i - 4, :, 1], dst.at[i], hsem.at[k, i])

    @pl.when(b == 0)
    def _():
        for i in range(n):
            get(g_hbm, g_ref, i, 0).start()
        zget(0, 0).start()
        zget(0, 1).start()
        for i in range(n):
            get(h_hbm, h_ref, i, 1).start()
        for i in range(n // 2 + 1):
            get(g_hbm, g_ref, i, 0).wait()

    def dots(i):
        ds[i % 2][...] = lax.dot_general(w2_ref[...], g_ref[i].reshape(tc, d), NT, preferred_element_type=F32)

    def elem(i):
        cols = pl.ds(i * tc, tc)
        off = (i * tc) % half
        for r in range(0, f, 32):
            a, da = gelu_parts(zs[i * tc // half][r:r + 32, off:off + tc])
            at[r:r + 32, cols] = a.astype(BF)
            dzt[r:r + 32, cols] = (ds[i % 2][r:r + 32, :] * da).astype(BF)

    zget(b, 0).wait()
    dots(0)
    for i in range(1, n // 2 + 1):
        dots(i)
        elem(i - 1)
    zget(b, 1).wait()

    @pl.when(b + 1 < nb)
    def _():
        zget(b + 1, 0).start()

    @pl.when(b == 0)
    def _():
        for i in range(n // 2 + 1, n):
            get(g_hbm, g_ref, i, 0).wait()
        for i in range(n):
            get(h_hbm, h_ref, i, 1).wait()
    for i in range(n // 2 + 1, n):
        dots(i)
        elem(i - 1)
    elem(n - 1)
    for j in range(0, d, BLK):
        cols = pl.ds(j, BLK)
        p1 = jnp.dot(dzt[...], h_ref[:, :, :, cols].reshape(t, BLK), preferred_element_type=F32)
        for r in range(0, BLK, 128):
            dw1_ref[pl.ds(j + r, 128), :] = p1[:, r:r + 128].T
        dw2_ref[:, cols] = jnp.dot(at[...], g_ref[:, :, :, cols].reshape(t, BLK), preferred_element_type=F32)

    @pl.when(b + 1 < nb)
    def _():
        zget(b + 1, 1).start()


def wgrad(z, w2, h, g, f=BLK, tc=BLK):
    ff, d = w2.shape
    t = z.shape[1]
    nb = z.shape[0] // f
    kept = pltpu.VMEM((t // tc, 4, tc // 4, d), BF)
    hbm = pl.BlockSpec(memory_space=pl.ANY)
    dma = pltpu.SemaphoreType.DMA
    return pl.pallas_call(
        wgrad_kernel,
        grid=(nb,),
        in_specs=[hbm, pl.BlockSpec((f, d), lambda i: (i, 0)), hbm, hbm],
        out_specs=[pl.BlockSpec((d, f), lambda i: (0, i)), pl.BlockSpec((f, d), lambda i: (i, 0))],
        out_shape=[jax.ShapeDtypeStruct((d, ff), F32), jax.ShapeDtypeStruct((ff, d), F32)],
        scratch_shapes=[kept] * 2 + [pltpu.VMEM((f, t), BF)] * 2 + [pltpu.VMEM((f, t // 2), F32)] * 2 + [pltpu.VMEM((f, tc), F32)] * 2
        + [dma((2, t // tc)), dma((2,))],
        compiler_params=pltpu.CompilerParams(vmem_limit_bytes=VMEM_BYTES, dimension_semantics=("arbitrary",)),
        cost_estimate=pl.CostEstimate(flops=6 * t * d * ff, bytes_accessed=10 * d * ff + 4 * t * d + 4 * t * ff, transcendentals=t * ff),
        name="wgrad",
    )(z, w2, h, g)


def share_kernel(w1_hbm, w2_hbm, y_in, dx_in, h_hbm, g_hbm, s1, s2, y, dx, h_ref, g_ref, at, dzt, win, wint, w2, hsem, gsem, wsem, *, tc):
    t = h_ref.shape[0]
    n = t // tc
    fs, ff = w2.shape[0], w2_hbm.shape[0]
    first = ff - 16 * fs + lax.axis_index("inner") * fs
    base = jnp.minimum((first // 128) * 128, ff - 256)
    c1 = pltpu.make_async_copy(w1_hbm.at[:, pl.ds(pl.multiple_of(base, 128), 256)], win, wsem.at[0])
    c2 = pltpu.make_async_copy(w2_hbm.at[pl.ds(pl.multiple_of(first, 32), fs), :], w2, wsem.at[1])
    c1.start()
    c2.start()
    y[...] = y_in[...]
    dx[...] = dx_in[...]

    def part(src, dst, sem, i):
        rows = pl.ds(i * tc if isinstance(i, int) else pl.multiple_of(i * tc, tc), tc)
        return pltpu.make_async_copy(src.at[rows], dst.at[rows], sem.at[i])
    for i in range(n):
        part(h_hbm, h_ref, hsem, i).start()
        part(g_hbm, g_ref, gsem, i).start()
    c1.wait()
    c2.wait()
    wint[...] = win[...].T
    w1t = wint.at[pl.ds(pl.multiple_of(first - base, 32), fs), :]

    @pl.loop(0, n)
    def _(i):
        rows = pl.ds(pl.multiple_of(i * tc, tc), tc)
        part(h_hbm, h_ref, hsem, i).wait()
        part(g_hbm, g_ref, gsem, i).wait()
        z = lax.dot_general(w1t[...], h_ref[rows, :], NT, preferred_element_type=F32)
        da = lax.dot_general(w2[...], g_ref[rows, :], NT, preferred_element_type=F32)
        a, dg = gelu_parts(z)
        at[:, rows] = a.astype(BF)
        dzt[:, rows] = (da * dg).astype(BF)

    @pl.loop(0, h_ref.shape[1] // BLK)
    def _(j):
        cols = pl.ds(pl.multiple_of(j * BLK, BLK), BLK)
        s1[:, cols] = jnp.dot(dzt[...], h_ref[:, cols], preferred_element_type=F32)
        s2[:, cols] = jnp.dot(at[...], g_ref[:, cols], preferred_element_type=F32)


def share(w1, w2, y, dx, h, g, fs, tc=1024):
    d = w2.shape[1]
    t = h.shape[0]
    vm = pl.BlockSpec(memory_space=pltpu.VMEM)
    hbm = pl.BlockSpec(memory_space=pl.ANY)
    dma = pltpu.SemaphoreType.DMA
    return pl.pallas_call(
        functools.partial(share_kernel, tc=tc),
        in_specs=[hbm, hbm, vm, vm, hbm, hbm],
        out_specs=[vm] * 4,
        out_shape=[jax.ShapeDtypeStruct((fs, d), F32)] * 2 + [jax.ShapeDtypeStruct(y.shape, BF)] * 2,
        scratch_shapes=[pltpu.VMEM((t, d), BF)] * 2 + [pltpu.VMEM((fs, t), BF)] * 2
        + [pltpu.VMEM((d, 256), BF), pltpu.VMEM((256, d), BF), pltpu.VMEM((fs, d), BF), dma((t // tc,)), dma((t // tc,)), dma((2,))],
        compiler_params=pltpu.CompilerParams(vmem_limit_bytes=VMEM_BYTES),
        cost_estimate=pl.CostEstimate(flops=16 * t * d * fs, bytes_accessed=4 * t * d, transcendentals=t * fs),
        name="share",
    )(w1, w2, y, dx, h, g)


def finish_kernel(s1, s2, dw1_in, dw2_in, dw1, dw2):
    del dw1_in, dw2_in
    for r in range(0, s1.shape[1], 256):
        dw1[pl.ds(r, 256), :] = s1[:, r:r + 256].T
    dw2[...] = s2[...]


def finish(s1, s2, dw1, dw2, f=256):
    n, d = s1.shape
    first = dw1.shape[1] // f - n // f
    hbm = pl.BlockSpec(memory_space=pl.ANY)
    row = pl.BlockSpec((f, d), lambda i: (i, 0))
    return pl.pallas_call(
        finish_kernel,
        grid=(n // f,),
        in_specs=[row, row, hbm, hbm],
        out_specs=[pl.BlockSpec((d, f), lambda i: (0, first + i)), pl.BlockSpec((f, d), lambda i: (first + i, 0))],
        out_shape=[jax.ShapeDtypeStruct(dw1.shape, F32), jax.ShapeDtypeStruct(dw2.shape, F32)],
        input_output_aliases={2: 0, 3: 1},
        compiler_params=pltpu.CompilerParams(vmem_limit_bytes=VMEM_BYTES, dimension_semantics=("arbitrary",)),
        cost_estimate=pl.CostEstimate(flops=n * d, bytes_accessed=16 * n * d, transcendentals=0),
        name="finish",
    )(s1, s2, dw1, dw2)


def solution(mesh):
    def body(x, g, w1, w2):
        w1, w2 = w1[0, 0], w2[0, 0]
        ff, d = w2.shape
        nz = NB * BLK
        fs = (ff - nz) // 16
        y, dx, h, gg, z = fb(x[0], g[0], w1, w2, nz)
        s1, s2, y, dx = share(w1, w2, y, dx, h.reshape(-1, d), gg.reshape(-1, d), fs)
        s1 = lax.all_gather(s1, "inner", axis=0, tiled=True)
        s2 = lax.all_gather(s2, "inner", axis=0, tiled=True)
        dw1, dw2 = wgrad(z, w2, h, gg)
        dw1, dw2 = finish(s1, s2, dw1, dw2)
        return y[None], dx[None], dw1[None, None], dw2[None, None]

    tok = P(("data", "stage"), "inner", None)
    wsp = P(None, "stage", None, None)
    dsp = P("data", "stage", None, None)
    return jax.shard_map(body, mesh=mesh, in_specs=(tok, tok, wsp, wsp), out_specs=(tok, tok, dsp, dsp), check_vma=False)
```
